512 devices in a mesh: fsdp: 64 (over y, z), dp: 8 (over x, core).
Axes of the slice: x: 4, y: 8, z: 8, core: 2. Of those that a mesh axis runs over, the one named last changes fastest.
Arguments:
- grad_parts: bfloat16 [8, 64, 512, 512], P('dp', None, 'fsdp'), may hold values from -2.5 to 2.5
- weights: float32 [64, 512, 512], P(None, 'fsdp', 'dp'), may hold values from -6 to 6
- left_stat: float32 [192, 512, 512], P('fsdp', 'dp'), may hold values from -6 to 6
- right_stat: float32 [192, 512, 512], P('fsdp', 'dp'), may hold values from -6 to 6
- left_codes: bfloat16 [192, 512, 512], P('fsdp'), may hold values from -1 to 1
- right_codes: bfloat16 [192, 512, 512], P('fsdp', 'dp'), may hold values from -1 to 1
- left_scales: float32 [192, 512], P('fsdp'), may hold values from 0.3 to 3
- right_scales: float32 [192, 512], P('fsdp', 'dp'), may hold values from 0.1 to 27
- owners: int32 [64], replicated, may hold values from 0 to 63, as said below
Outputs:
- new_weights: float32 [64, 512, 512], P(None, 'fsdp', 'dp')
- new_left_stat: float32 [192, 512, 512], P('fsdp', 'dp')
- new_right_stat: float32 [192, 512, 512], P('fsdp', 'dp')
The draws below stay inside these ranges and needn't reach their ends.
Inputs may be any that keep to these rules, and one draw needn't show every extreme that they name: `owners`: each owner is named by at most 3 blocks, and some owner by exactly 3 blocks.
All inputs are finite; a program needn't handle non-finite values.
Results may differ from the reference program's by a relative error of at most 0.0095.
Values may be sent and summed in bfloat16 or wider, within the bound.
No kernel may reach another device: no remote copies, remote signals or barrier semaphores. Data moves between devices by JAX's collectives and lax.ppermute only.
A program may use at most 64 MiB of HBM per device.

```python
import math
import jax
import jax.numpy as jnp
from jax import lax

B = 512
MOST = 3
NB = 64
SLOTS = 192
N_DP = 8


def draw_owners(key, part):
    first_key, second_key, third_key = jax.random.split(jax.random.fold_in(key, 7), 3)
    shuffle = jax.random.permutation(first_key, NB).astype(jnp.int32)
    heavy_count = jax.random.randint(second_key, (), 1, NB // (2 * MOST) + 1)
    positions = jnp.arange(NB, dtype=jnp.int32)
    counts = jnp.where(positions < heavy_count, MOST, jnp.where(positions < MOST * heavy_count, 0, 1)).astype(jnp.int32)
    bounds = jnp.cumsum(counts)
    picked = jnp.sum((bounds[None, :] <= positions[:, None]).astype(jnp.int32), axis=1)
    ordered = shuffle[picked]
    return ordered[jax.random.permutation(third_key, NB)].astype(jnp.int32)


def draw_right_scales(key, part):
    scale_key = jax.random.fold_in(key, 11)
    row_frac = jnp.arange(B, dtype=jnp.float32) / (B - 1)
    bottom = jnp.log(0.3)
    growth = jnp.log(3.0)
    uniform_log = jax.random.uniform(scale_key, (SLOTS, B), jnp.float32, bottom, jnp.log(3.0))
    return jnp.exp(uniform_log + growth * row_frac[None, :]).astype(jnp.float32)


def shard_levels(own_key, extent, cuts, smallest, high):
    gain, own = 1.0, jax.random.fold_in(own_key, 6)
    for axis_at, parts in cuts:
        steps = jnp.exp(jax.random.uniform(jax.random.fold_in(own, axis_at), (parts,), jnp.float32, smallest / len(cuts), high / len(cuts)))
        gain = gain * jnp.repeat(steps, extent[axis_at] // parts).reshape([-1 if axis == axis_at else 1 for axis in range(len(extent))])
    return gain


def scatter_about(key, shape, spread, limit, cuts=(), kind=jnp.bfloat16):
    drawn = spread * jax.random.normal(key, shape, jnp.float32)
    if cuts:
        drawn = drawn * shard_levels(key, shape, cuts, -0.22, 0.18)
    return jnp.clip(drawn, -limit, limit).astype(kind)


def setup_inputs(seed: int = 0) -> dict:
    streams_of = jax.random.split(jax.random.key(seed), 10)
    grad_parts = scatter_about(streams_of[0], (N_DP, NB, B, B), 0.35, 2.5, ((0, 8), (2, 64)))
    weights = scatter_about(streams_of[1], (NB, B, B), 1.0, 6.0, ((1, 64), (2, 8)), jnp.float32)
    left_stat = scatter_about(streams_of[2], (SLOTS, B, B), 1.0, 6.0, ((0, 64), (1, 8)), jnp.float32)
    right_stat = scatter_about(streams_of[3], (SLOTS, B, B), 1.0, 6.0, ((0, 64), (1, 8)), jnp.float32)
    left_codes = jnp.clip(jax.random.uniform(streams_of[4], (SLOTS, B, B), jnp.float32, -1.0, 1.0) * shard_levels(streams_of[4], (SLOTS, B, B), ((0, 64),), -0.4, 0.0), -1.0, 1.0).astype(jnp.bfloat16)
    right_codes = jnp.clip(jax.random.uniform(streams_of[5], (SLOTS, B, B), jnp.float32, -1.0, 1.0) * shard_levels(streams_of[5], (SLOTS, B, B), ((0, 64), (1, 8)), -0.4, 0.0), -1.0, 1.0).astype(jnp.bfloat16)
    left_scales = jnp.clip(jnp.exp(math.log(3.0) - 2.3025851 * jax.random.uniform(streams_of[6], (SLOTS, B), jnp.float32) ** shard_levels(streams_of[6], (SLOTS, B), ((0, 64),), -0.2, 0.2)), 0.3, 3.0)
    right_scales = draw_right_scales(jax.random.fold_in(streams_of[9], 71), 0)
    owners = draw_owners(jax.random.fold_in(streams_of[9], 71), 0)
    return {"grad_parts": grad_parts, "weights": weights, "left_stat": left_stat, "right_stat": right_stat, "left_codes": left_codes, "right_codes": right_codes, "left_scales": left_scales, "right_scales": right_scales, "owners": owners}


stat_decay = 0.95
step_size = 0.5
epsilon = 1e-06

def slot_table(owners, capacity):
    count = owners.shape[0]
    index = jnp.arange(count, dtype=jnp.int32)
    earlier = (owners[:, None] == owners[None, :]) & (index[None, :] < index[:, None])
    rank = lax.optimization_barrier(jnp.sum(earlier.astype(jnp.int32), axis=1)).astype(jnp.int32)
    return (owners * capacity + rank).astype(jnp.int32)

def reference(grad_parts, weights, left_stat, right_stat, left_codes, right_codes, left_scales, right_scales, owners):
    grad = lax.optimization_barrier(jnp.sum(grad_parts.astype(jnp.float32), axis=0)).astype(jnp.bfloat16)
    slot_of = slot_table(owners, MOST)
    slot_ids = jnp.arange(SLOTS, dtype=jnp.int32)
    matches = slot_of[None, :] == slot_ids[:, None]
    block_ids = jnp.arange(NB, dtype=jnp.int32)
    source = lax.optimization_barrier(jnp.sum(jnp.where(matches, block_ids[None, :], 0), axis=1)).astype(jnp.int32)
    filled = jnp.any(matches, axis=1)

    def per_slot(slot_index):
        taken = lax.dynamic_index_in_dim(grad, source[slot_index], 0, keepdims=False)
        block_grad = jnp.where(filled[slot_index], taken, jnp.zeros_like(taken))
        gram_left = jnp.dot(block_grad, block_grad.T, preferred_element_type=jnp.float32)
        gram_right = jnp.dot(block_grad.T, block_grad, preferred_element_type=jnp.float32)
        left_new = stat_decay * left_stat[slot_index] + (1.0 - stat_decay) * gram_left
        right_new = stat_decay * right_stat[slot_index] + (1.0 - stat_decay) * gram_right
        left_factor = (left_codes[slot_index].astype(jnp.float32) * left_scales[slot_index][:, None]).astype(jnp.bfloat16)
        right_factor = (right_codes[slot_index].astype(jnp.float32) * right_scales[slot_index][:, None]).astype(jnp.bfloat16)
        mixed = jnp.dot(block_grad, right_factor.T, preferred_element_type=jnp.float32).astype(jnp.bfloat16)
        precond = jnp.dot(left_factor, mixed, preferred_element_type=jnp.float32)
        grad_squares = jnp.sum(jnp.square(block_grad.astype(jnp.float32)))
        pre_squares = jnp.sum(precond * precond)
        graft_ratio = jnp.sqrt(grad_squares) * lax.rsqrt(pre_squares + epsilon)
        return (left_new, right_new, step_size * graft_ratio * precond)
    left_new, right_new, updates = lax.map(per_slot, slot_ids)
    new_weights = weights - jnp.take(updates, slot_of, axis=0)
    return (new_weights, left_new, right_new)
```

```python
import jax
import jax.numpy as jnp
from jax import lax
from jax.experimental import pallas as pl
from jax.experimental.pallas import tpu as pltpu
from jax.sharding import Mesh
from jax.sharding import PartitionSpec as P

stat_decay = 0.95
step_size = 0.5
epsilon = 1e-06

bf16 = jnp.bfloat16
f32 = jnp.float32
LANES = 128
VMEM_GRANT = 16 * 1024 * 1024


def iota(shape, dim):
    return lax.broadcasted_iota(jnp.int32, shape, dim)


def dot(a, b, ca=1, cb=0):
    return lax.dot_general(a, b, (((ca,), (cb,)), ((), ())), preferred_element_type=f32)


def onehot(mask):
    return jnp.where(mask, 1.0, 0.0).astype(bf16)


def natural_row(order, first_half):
    half = (order // 256 + first_half) % 2
    return 8 * (order % 64) + 4 * half + (order // 64) % 4


def vmem(n):
    return [pl.BlockSpec(memory_space=pltpu.VMEM)] * n


SMEM = pl.BlockSpec(memory_space=pltpu.SMEM)
ANY = pl.BlockSpec(memory_space=pl.ANY)


def call(kernel, ins, outs, args):
    single = not isinstance(outs, (list, tuple))
    shapes = [outs] if single else list(outs)
    got = pl.pallas_call(
        kernel,
        out_shape=shapes,
        in_specs=ins,
        out_specs=vmem(len(shapes)),
        compiler_params=pltpu.CompilerParams(vmem_limit_bytes=VMEM_GRANT),
    )(*args)
    return got[0] if single else got


def sds(shape, dtype):
    return jax.ShapeDtypeStruct(shape, dtype)


def split_kernel(x_ref, out_ref):
    rows = x_ref.shape[0]
    target = natural_row(iota((rows, rows), 0), 0)
    perm = onehot(target == iota((rows, rows), 1))
    moved = dot(perm, x_ref[...]).astype(bf16)
    for x in range(4):
        for c in range(2):
            out_ref[2 * x + c] = moved[256 * c : 256 * c + 256, LANES * x : LANES * x + LANES]


def route_kernel(parts_ref, slot_ref, out_ref):
    total = parts_ref[0].astype(f32)
    for s in range(1, 8):
        total = total + parts_ref[s].astype(f32)
    total = total.astype(bf16)
    wide = jnp.concatenate([total[64 * r : 64 * r + 64] for r in range(4)], axis=1)
    slot = slot_ref[...]
    for k in range(3):
        pick = onehot(slot == 3 * iota((64, 64), 0) + k)
        out_ref[:, 512 * k : 512 * k + 512] = dot(pick, wide).astype(bf16)


def left_kernel(core_ref, lf_ref, after_ref, out_ref):
    back = onehot(natural_row(iota((512, 512), 0), 0) == iota((512, 512), 1))
    cols = onehot(natural_row(iota((512, 512), 1), core_ref[0]) == iota((512, 512), 0))
    for k in range(3):
        rows = dot(back, lf_ref[k]).astype(bf16)
        out_ref[k] = dot(rows, cols).astype(bf16)


def main_kernel(own_ref, other_ref, rf_ref, left_ref, g_ref, p_ref, sq_ref, gs_ref):
    lane = iota((8, LANES), 1)
    squares = jnp.zeros((8, LANES), f32)
    grad_squares = jnp.zeros((8, LANES), f32)
    for k in range(3):
        for s, src in enumerate((own_ref, other_ref)):
            for r in range(4):
                at = LANES * (4 * k + r)
                for x in range(4):
                    row = 256 * s + 64 * r
                    g_ref[k, row : row + 64, LANES * x : LANES * x + LANES] = src[
                        x, :, at : at + LANES
                    ]
        g = g_ref[k]
        rf = rf_ref[k]
        wide = jnp.concatenate([rf, jnp.zeros((128, 512), bf16), rf], axis=0)
        mixed = dot(g, wide, 1, 1).astype(bf16)
        pre = dot(left_ref[k, :256], mixed[:, :128]) + dot(left_ref[k, 256:], mixed[:, 128:])
        for t in range(4):
            at = 512 * k + LANES * t
            p_ref[:, at : at + LANES] = pre[64 * t : 64 * t + 64]
        squares = jnp.where(lane == k, jnp.sum(pre * pre), squares)
        gf = g.astype(f32)
        grad_squares = jnp.where(lane == k, jnp.sum(gf * gf), grad_squares)
    sq_ref[...] = squares
    gs_ref[...] = grad_squares


def scale_kernel(sq_ref, gs_ref, p_ref, out_ref):
    total = jnp.sum(sq_ref[...], axis=0, keepdims=True)
    ratio = step_size * jnp.sqrt(gs_ref[0:1, :]) * lax.rsqrt(total + epsilon)
    for k in range(3):
        span = slice(512 * k, 512 * k + 512)
        out_ref[:, span] = (p_ref[:, span] * ratio[:, k : k + 1]).astype(bf16)


def right_kernel(replica_ref, g_ref, stat_ref, out_ref):
    pick = onehot(iota((64, 512), 1) == 64 * replica_ref[0] + iota((64, 512), 0))
    for k in range(3):
        g = g_ref[k]
        cols = dot(pick, g, 1, 1).astype(bf16)
        out_ref[k] = stat_decay * stat_ref[k] + (1.0 - stat_decay) * dot(cols, g)


def gram_left_kernel(replica_ref, core_ref, g_ref, stat_ref, after_ref, out_ref):
    core = core_ref[0]
    order = natural_row(iota((512, 512), 1), core)
    back = onehot(order == iota((512, 512), 0))
    mine = onehot(
        natural_row(iota((64, 512), 1), core) == 64 * replica_ref[0] + iota((64, 512), 0)
    )
    for k in range(3):
        g = g_ref[k]
        rows = dot(mine, g).astype(bf16)
        whole = dot(back, g).astype(bf16)
        out_ref[k] = stat_decay * stat_ref[k] + (1.0 - stat_decay) * dot(rows, whole, 1, 1)


def final_kernel(ret_ref, slot_ref, w_ref, out_ref):
    slot = slot_ref[...]
    update = jnp.zeros((64, 512), f32)
    for k in range(3):
        pick = onehot(slot == 3 * iota((64, 64), 1) + k)
        update = update + dot(pick, ret_ref[:, 512 * k : 512 * k + 512])
    for t in range(4):
        for half in range(2):
            row = 4 * half + t
            at = LANES * t + 64 * half
            out_ref[:, row, :] = w_ref[:, row, :] - update[:, at : at + 64]


def slot_table(owners, capacity):
    count = owners.shape[0]
    index = jnp.arange(count, dtype=jnp.int32)
    earlier = (owners[:, None] == owners[None, :]) & (index[None, :] < index[:, None])
    rank = jnp.sum(earlier.astype(jnp.int32), axis=1)
    return owners * capacity + rank


def exchange(x, axis):
    return lax.all_to_all(x, axis, split_axis=0, concat_axis=0, tiled=True)


def local(
    grad_parts,
    weights,
    left_stat,
    right_stat,
    left_codes,
    right_codes,
    left_scales,
    right_scales,
    owners,
):
    core = lax.axis_index("core").astype(jnp.int32)
    replica = (2 * lax.axis_index("x") + core).astype(jnp.int32)[None]
    core = core[None]
    slot_of = slot_table(owners, 3)

    split = call(split_kernel, vmem(1), sds((8, 256, 128), bf16), (grad_parts.reshape(512, 512),))
    parts = exchange(split, ("x", "core"))
    routed = call(
        route_kernel, vmem(2), sds((64, 1536), bf16), (parts, slot_of.reshape(1, 64))
    )
    arrived = exchange(routed.reshape(64, 2, 768), "fsdp")

    left_factor = (left_codes.astype(f32) * left_scales[:, :, None]).astype(bf16)
    right_factor = (right_codes.astype(f32) * right_scales[:, :, None]).astype(bf16)
    left = call(
        left_kernel, [SMEM, *vmem(1), ANY], sds((3, 512, 512), bf16), (core, left_factor, routed)
    )

    own = exchange(jnp.broadcast_to(arrived, (4, 64, 2, 768)).reshape(256, 2, 768), "x")
    other = lax.ppermute(own, "core", [(0, 1), (1, 0)])
    grad, pre, squares, grad_squares = call(
        main_kernel,
        vmem(4),
        [
            sds((3, 512, 512), bf16),
            sds((64, 1536), f32),
            sds((8, 128), f32),
            sds((8, 128), f32),
        ],
        (own.reshape(4, 64, 1536), other.reshape(4, 64, 1536), right_factor, left),
    )
    all_squares = exchange(squares.reshape(8, 1, 128), ("x", "core")).reshape(8, 128)
    right_new = call(
        right_kernel, [SMEM, *vmem(2)], sds((3, 64, 512), f32), (replica, grad, right_stat)
    )
    scaled = call(
        scale_kernel, vmem(3), sds((64, 1536), bf16), (all_squares, grad_squares, pre)
    )
    returned = exchange(scaled.reshape(64, 2, 768), "fsdp").reshape(64, 1536)
    left_new = call(
        gram_left_kernel,
        [SMEM, SMEM, *vmem(2), ANY],
        sds((3, 64, 512), f32),
        (replica, core, grad, left_stat, scaled),
    )
    new_weights = call(
        final_kernel,
        vmem(3),
        sds((64, 8, 64), f32),
        (returned, slot_of.reshape(64, 1), weights),
    )
    return (new_weights, left_new, right_new)


def solution(mesh):
    grid = Mesh(mesh.devices.reshape(64, 4, 2), ("fsdp", "x", "core"))
    dp = ("x", "core")
    return jax.shard_map(
        local,
        mesh=grid,
        in_specs=(
            P(dp, None, "fsdp", None),
            P(None, "fsdp", dp),
            P("fsdp", dp, None),
            P("fsdp", dp, None),
            P("fsdp", None, None),
            P("fsdp", dp, None),
            P("fsdp", None),
            P("fsdp", dp),
            P(),
        ),
        out_specs=(P(None, "fsdp", dp), P("fsdp", dp, None), P("fsdp", dp, None)),
        check_vma=False,
    )
```

```python
import jax
import jax.numpy as jnp
from jax import lax
from jax.experimental import pallas as pl
from jax.experimental.pallas import tpu as pltpu
from jax.sharding import Mesh
from jax.sharding import PartitionSpec as P

stat_decay = 0.95
step_size = 0.5
epsilon = 1e-06

bf16 = jnp.bfloat16
f32 = jnp.float32
LANES = 128
VMEM_GRANT = 16 * 1024 * 1024


def iota(shape, dim):
    return lax.broadcasted_iota(jnp.int32, shape, dim)


def dot(a, b, ca=1, cb=0):
    return lax.dot_general(a, b, (((ca,), (cb,)), ((), ())), preferred_element_type=f32)


def onehot(mask):
    return jnp.where(mask, 1.0, 0.0).astype(bf16)


def natural_row(order, first_half):
    half = (order // 256 + first_half) % 2
    return 8 * (order % 64) + 4 * half + (order // 64) % 4


def vmem(n):
    return [pl.BlockSpec(memory_space=pltpu.VMEM)] * n


SMEM = pl.BlockSpec(memory_space=pltpu.SMEM)
ANY = pl.BlockSpec(memory_space=pl.ANY)


def call(kernel, ins, outs, args):
    single = not isinstance(outs, (list, tuple))
    shapes = [outs] if single else list(outs)
    got = pl.pallas_call(
        kernel,
        out_shape=shapes,
        in_specs=ins,
        out_specs=vmem(len(shapes)),
        compiler_params=pltpu.CompilerParams(vmem_limit_bytes=VMEM_GRANT),
    )(*args)
    return got[0] if single else got


def sds(shape, dtype):
    return jax.ShapeDtypeStruct(shape, dtype)


CHUNKS = 4


def split_kernel(x_ref, out_ref, x_buf, out_buf, in_sem, out_sem):
    rows = x_buf.shape[1]
    per = rows // 8

    def arrival(i):
        return pltpu.make_async_copy(x_ref.at[pl.ds(rows * i, rows)], x_buf.at[i], in_sem.at[i])

    def leaving(i):
        target = out_ref.at[:, :, pl.ds(per * i, per)]
        return pltpu.make_async_copy(out_buf.at[i], target, out_sem.at[i])

    for i in range(CHUNKS):
        arrival(i).start()
    order = iota((rows, rows), 0)
    half, r, block = order // (4 * per), (order // per) % 4, order % per
    perm = onehot(8 * block + 4 * half + r == iota((rows, rows), 1))
    for i in range(CHUNKS):
        arrival(i).wait()
        moved = dot(perm, x_buf[i]).astype(bf16)
        for x in range(4):
            for c in range(2):
                for r in range(4):
                    at = (4 * c + r) * per
                    piece = moved[at : at + per, LANES * x : LANES * x + LANES]
                    out_buf[i, 2 * x + c, r] = piece
        leaving(i).start()
    for i in range(CHUNKS):
        leaving(i).wait()


def split(x):
    rows = 512 // CHUNKS
    hbm = pl.BlockSpec(memory_space=pltpu.HBM)
    return pl.pallas_call(
        split_kernel,
        out_shape=sds((8, 4, 64, 128), bf16),
        in_specs=[hbm],
        out_specs=hbm,
        scratch_shapes=[
            pltpu.VMEM((CHUNKS, rows, 512), bf16),
            pltpu.VMEM((CHUNKS, 8, 4, rows // 8, 128), bf16),
            pltpu.SemaphoreType.DMA((CHUNKS,)),
            pltpu.SemaphoreType.DMA((CHUNKS,)),
        ],
        compiler_params=pltpu.CompilerParams(vmem_limit_bytes=VMEM_GRANT),
    )(x).reshape(8, 256, 128)


def route_kernel(parts_ref, slot_ref, out_ref):
    total = parts_ref[0].astype(f32)
    for s in range(1, 8):
        total = total + parts_ref[s].astype(f32)
    total = total.astype(bf16)
    wide = jnp.concatenate([total[64 * r : 64 * r + 64] for r in range(4)], axis=1)
    slot = slot_ref[...]
    for k in range(3):
        pick = onehot(slot == 3 * iota((64, 64), 0) + k)
        out_ref[:, 512 * k : 512 * k + 512] = dot(pick, wide).astype(bf16)


def left_kernel(core_ref, lf_ref, after_ref, out_ref):
    back = onehot(natural_row(iota((512, 512), 0), 0) == iota((512, 512), 1))
    cols = onehot(natural_row(iota((512, 512), 1), core_ref[0]) == iota((512, 512), 0))
    for k in range(3):
        rows = dot(back, lf_ref[k]).astype(bf16)
        out_ref[k] = dot(rows, cols).astype(bf16)


def main_kernel(own_ref, other_ref, rf_ref, left_ref, g_ref, p_ref, sq_ref, gs_ref):
    lane = iota((8, LANES), 1)
    squares = jnp.zeros((8, LANES), f32)
    grad_squares = jnp.zeros((8, LANES), f32)
    for k in range(3):
        for s, src in enumerate((own_ref, other_ref)):
            for r in range(4):
                at = LANES * (4 * k + r)
                for x in range(4):
                    row = 256 * s + 64 * r
                    g_ref[k, row : row + 64, LANES * x : LANES * x + LANES] = src[
                        x, :, at : at + LANES
                    ]
        g = g_ref[k]
        rf = rf_ref[k]
        wide = jnp.concatenate([rf, jnp.zeros((128, 512), bf16), rf], axis=0)
        mixed = dot(g, wide, 1, 1).astype(bf16)
        pre = dot(left_ref[k, :256], mixed[:, :128]) + dot(left_ref[k, 256:], mixed[:, 128:])
        for t in range(4):
            at = 512 * k + LANES * t
            p_ref[:, at : at + LANES] = pre[64 * t : 64 * t + 64]
        squares = jnp.where(lane == k, jnp.sum(pre * pre), squares)
        gf = g.astype(f32)
        grad_squares = jnp.where(lane == k, jnp.sum(gf * gf), grad_squares)
    sq_ref[...] = squares
    gs_ref[...] = grad_squares


def scale_kernel(sq_ref, gs_ref, p_ref, out_ref):
    total = jnp.sum(sq_ref[...], axis=0, keepdims=True)
    ratio = step_size * jnp.sqrt(gs_ref[0:1, :]) * lax.rsqrt(total + epsilon)
    for k in range(3):
        span = slice(512 * k, 512 * k + 512)
        out_ref[:, span] = (p_ref[:, span] * ratio[:, k : k + 1]).astype(bf16)


def right_kernel(replica_ref, g_ref, stat_ref, out_ref):
    pick = onehot(iota((64, 512), 1) == 64 * replica_ref[0] + iota((64, 512), 0))
    for k in range(3):
        g = g_ref[k]
        cols = dot(pick, g, 1, 1).astype(bf16)
        out_ref[k] = stat_decay * stat_ref[k] + (1.0 - stat_decay) * dot(cols, g)


def gram_left_kernel(replica_ref, core_ref, g_ref, stat_ref, after_ref, out_ref):
    core = core_ref[0]
    order = natural_row(iota((512, 512), 1), core)
    back = onehot(order == iota((512, 512), 0))
    mine = onehot(
        natural_row(iota((64, 512), 1), core) == 64 * replica_ref[0] + iota((64, 512), 0)
    )
    for k in range(3):
        g = g_ref[k]
        rows = dot(mine, g).astype(bf16)
        whole = dot(back, g).astype(bf16)
        out_ref[k] = stat_decay * stat_ref[k] + (1.0 - stat_decay) * dot(rows, whole, 1, 1)


def final_kernel(ret_ref, slot_ref, w_ref, out_ref):
    slot = slot_ref[...]
    update = jnp.zeros((64, 512), f32)
    for k in range(3):
        pick = onehot(slot == 3 * iota((64, 64), 1) + k)
        update = update + dot(pick, ret_ref[:, 512 * k : 512 * k + 512])
    for t in range(4):
        for half in range(2):
            row = 4 * half + t
            at = LANES * t + 64 * half
            out_ref[:, row, :] = w_ref[:, row, :] - update[:, at : at + 64]


def slot_table(owners, capacity):
    count = owners.shape[0]
    index = jnp.arange(count, dtype=jnp.int32)
    earlier = (owners[:, None] == owners[None, :]) & (index[None, :] < index[:, None])
    rank = jnp.sum(earlier.astype(jnp.int32), axis=1)
    return owners * capacity + rank


def exchange(x, axis):
    return lax.all_to_all(x, axis, split_axis=0, concat_axis=0, tiled=True)


def local(
    grad_parts,
    weights,
    left_stat,
    right_stat,
    left_codes,
    right_codes,
    left_scales,
    right_scales,
    owners,
):
    core = lax.axis_index("core").astype(jnp.int32)
    replica = (2 * lax.axis_index("x") + core).astype(jnp.int32)[None]
    core = core[None]
    slot_of = slot_table(owners, 3)

    parts = exchange(split(grad_parts.reshape(512, 512)), ("x", "core"))
    routed = call(
        route_kernel, vmem(2), sds((64, 1536), bf16), (parts, slot_of.reshape(1, 64))
    )
    arrived = exchange(routed.reshape(64, 2, 768), "fsdp").reshape(64, 1536)

    left_factor = (left_codes.astype(f32) * left_scales[:, :, None]).astype(bf16)
    right_factor = (right_codes.astype(f32) * right_scales[:, :, None]).astype(bf16)
    left = call(
        left_kernel, [SMEM, *vmem(1), ANY], sds((3, 512, 512), bf16), (core, left_factor, routed)
    )

    own = exchange(jnp.broadcast_to(arrived, (4, 64, 1536)), "x")
    other = lax.ppermute(own, "core", [(0, 1), (1, 0)])
    grad, pre, squares, grad_squares = call(
        main_kernel,
        vmem(4),
        [
            sds((3, 512, 512), bf16),
            sds((64, 1536), f32),
            sds((8, 128), f32),
            sds((8, 128), f32),
        ],
        (own, other, right_factor, left),
    )
    all_squares = exchange(squares.reshape(8, 1, 128), ("x", "core")).reshape(8, 128)
    right_new = call(
        right_kernel, [SMEM, *vmem(2)], sds((3, 64, 512), f32), (replica, grad, right_stat)
    )
    scaled = call(
        scale_kernel, vmem(3), sds((64, 1536), bf16), (all_squares, grad_squares, pre)
    )
    returned = exchange(scaled.reshape(64, 2, 768), "fsdp").reshape(64, 1536)
    left_new = call(
        gram_left_kernel,
        [SMEM, SMEM, *vmem(2), ANY],
        sds((3, 64, 512), f32),
        (replica, core, grad, left_stat, scaled),
    )
    new_weights = call(
        final_kernel,
        vmem(3),
        sds((64, 8, 64), f32),
        (returned, slot_of.reshape(64, 1), weights),
    )
    return (new_weights, left_new, right_new)


def solution(mesh):
    grid = Mesh(mesh.devices.reshape(64, 4, 2), ("fsdp", "x", "core"))
    dp = ("x", "core")
    return jax.shard_map(
        local,
        mesh=grid,
        in_specs=(
            P(dp, None, "fsdp", None),
            P(None, "fsdp", dp),
            P("fsdp", dp, None),
            P("fsdp", dp, None),
            P("fsdp", None, None),
            P("fsdp", dp, None),
            P("fsdp", None),
            P("fsdp", dp),
            P(),
        ),
        out_specs=(P(None, "fsdp", dp), P("fsdp", dp, None), P("fsdp", dp, None)),
        check_vma=False,
    )
```

```python
import jax
import jax.numpy as jnp
from jax import lax
from jax.experimental import pallas as pl
from jax.experimental.pallas import tpu as pltpu
from jax.sharding import Mesh
from jax.sharding import PartitionSpec as P

stat_decay = 0.95
step_size = 0.5
epsilon = 1e-06

bf16 = jnp.bfloat16
f32 = jnp.float32
LANES = 128
VMEM_GRANT = 16 * 1024 * 1024


def iota(shape, dim):
    return lax.broadcasted_iota(jnp.int32, shape, dim)


def dot(a, b, ca=1, cb=0):
    return lax.dot_general(a, b, (((ca,), (cb,)), ((), ())), preferred_element_type=f32)


def onehot(mask):
    return jnp.where(mask, 1.0, 0.0).astype(bf16)


def natural_row(order, first_half):
    half = (order // 256 + first_half) % 2
    return 8 * (order % 64) + 4 * half + (order // 64) % 4


def vmem(n):
    return [pl.BlockSpec(memory_space=pltpu.VMEM)] * n


SMEM = pl.BlockSpec(memory_space=pltpu.SMEM)
ANY = pl.BlockSpec(memory_space=pl.ANY)


def call(kernel, ins, outs, args):
    single = not isinstance(outs, (list, tuple))
    shapes = [outs] if single else list(outs)
    got = pl.pallas_call(
        kernel,
        out_shape=shapes,
        in_specs=ins,
        out_specs=vmem(len(shapes)),
        compiler_params=pltpu.CompilerParams(vmem_limit_bytes=VMEM_GRANT),
    )(*args)
    return got[0] if single else got


def sds(shape, dtype):
    return jax.ShapeDtypeStruct(shape, dtype)


CHUNKS = 4


def split_kernel(x_ref, out_ref, buf, sem):
    rows = 512 // CHUNKS
    per = rows // 8

    def leaving(i):
        return pltpu.make_async_copy(buf.at[i], out_ref.at[:, :, pl.ds(per * i, per)], sem.at[i])

    order = iota((rows, rows), 0)
    half, r, block = order // (4 * per), (order // per) % 4, order % per
    perm = onehot(8 * block + 4 * half + r == iota((rows, rows), 1))
    for i in range(CHUNKS):
        moved = dot(perm, x_ref[rows * i : rows * i + rows]).astype(bf16)
        for x in range(4):
            for c in range(2):
                for r in range(4):
                    at = (4 * c + r) * per
                    piece = moved[at : at + per, LANES * x : LANES * x + LANES]
                    buf[i, 2 * x + c, r] = piece
        leaving(i).start()
    for i in range(CHUNKS):
        leaving(i).wait()


def split(x):
    return pl.pallas_call(
        split_kernel,
        out_shape=sds((8, 4, 64, 128), bf16),
        in_specs=vmem(1),
        out_specs=ANY,
        scratch_shapes=[
            pltpu.VMEM((CHUNKS, 8, 4, 64 // CHUNKS, 128), bf16),
            pltpu.SemaphoreType.DMA((CHUNKS,)),
        ],
        compiler_params=pltpu.CompilerParams(vmem_limit_bytes=VMEM_GRANT),
    )(x)


def route_kernel(parts_ref, slot_ref, after_ref, out_ref):
    total = parts_ref[0].astype(f32)
    for s in range(1, 8):
        total = total + parts_ref[s].astype(f32)
    total = total.astype(bf16)
    wide = jnp.concatenate([total[64 * r : 64 * r + 64] for r in range(4)], axis=1)
    slot = slot_ref[...]
    for k in range(3):
        pick = onehot(slot == 3 * iota((64, 64), 0) + k)
        out_ref[:, 512 * k : 512 * k + 512] = dot(pick, wide).astype(bf16)


def left_kernel(core_ref, lf_ref, after_ref, out_ref):
    back = onehot(natural_row(iota((512, 512), 0), 0) == iota((512, 512), 1))
    cols = onehot(natural_row(iota((512, 512), 1), core_ref[0]) == iota((512, 512), 0))
    for k in range(3):
        rows = dot(back, lf_ref[k]).astype(bf16)
        out_ref[k] = dot(rows, cols).astype(bf16)


def spread_kernel(piece_ref, out_ref):
    for q in range(4):
        for kr in range(12):
            tile = piece_ref[16 * q : 16 * q + 16, LANES * kr : LANES * kr + LANES]
            for x in range(4):
                at = 192 * q + 16 * kr
                out_ref[x, at : at + 16] = tile


def half_products(at, src_ref, rf_ref, left_ref, g_ref):
    lane = iota((8, LANES), 1)
    grad_squares = jnp.zeros((8, LANES), f32)
    products = []
    for k in range(3):
        for x in range(4):
            for q in range(4):
                for r in range(4):
                    row = 64 * r + 16 * q
                    g_ref[k, row : row + 16, LANES * x : LANES * x + LANES] = src_ref[
                        x, pl.ds(192 * q + 16 * (4 * k + r), 16)
                    ]
        g = g_ref[k]
        rf = rf_ref[k]
        wide = jnp.concatenate([rf, jnp.zeros((128, 512), bf16), rf], axis=0)
        mixed = dot(g, wide, 1, 1).astype(bf16)
        pre = dot(left_ref[k, :256, at : at + 256], mixed[:, :128])
        products.append(pre + dot(left_ref[k, 256:, at : at + 256], mixed[:, 128:]))
        gf = g.astype(f32)
        grad_squares = jnp.where(lane == k, jnp.sum(gf * gf), grad_squares)
    return products, grad_squares


def own_kernel(own_ref, rf_ref, left_ref, g_ref, p_ref, gs_ref):
    products, grad_squares = half_products(0, own_ref, rf_ref, left_ref, g_ref)
    for k in range(3):
        p_ref[k] = products[k]
    gs_ref[...] = grad_squares


def other_kernel(
    other_ref, rf_ref, left_ref, own_p_ref, own_gs_ref, g_ref, p_ref, sq_ref, gs_ref
):
    products, grad_squares = half_products(256, other_ref, rf_ref, left_ref, g_ref)
    lane = iota((8, LANES), 1)
    squares = jnp.zeros((8, LANES), f32)
    for k in range(3):
        pre = own_p_ref[k] + products[k]
        for t in range(4):
            at = 512 * k + LANES * t
            p_ref[:, at : at + LANES] = pre[64 * t : 64 * t + 64]
        squares = jnp.where(lane == k, jnp.sum(pre * pre), squares)
    sq_ref[...] = squares
    gs_ref[...] = own_gs_ref[...] + grad_squares


def scale_kernel(sq_ref, gs_ref, p_ref, out_ref):
    total = jnp.sum(sq_ref[...], axis=0, keepdims=True)
    ratio = step_size * jnp.sqrt(gs_ref[0:1, :]) * lax.rsqrt(total + epsilon)
    for k in range(3):
        span = slice(512 * k, 512 * k + 512)
        out_ref[:, span] = (p_ref[:, span] * ratio[:, k : k + 1]).astype(bf16)


def right_kernel(replica_ref, own_ref, other_ref, stat_ref, out_ref):
    pick = onehot(iota((64, 512), 1) == 64 * replica_ref[0] + iota((64, 512), 0))
    for k in range(3):
        g = jnp.concatenate([own_ref[k], other_ref[k]], axis=0)
        cols = dot(pick, g, 1, 1).astype(bf16)
        out_ref[k] = stat_decay * stat_ref[k] + (1.0 - stat_decay) * dot(cols, g)


def gram_left_kernel(
    replica_ref, core_ref, own_ref, other_ref, stat_ref, after_ref, out_ref
):
    core = core_ref[0]
    order = natural_row(iota((512, 512), 1), core)
    back = onehot(order == iota((512, 512), 0))
    mine = onehot(
        natural_row(iota((64, 512), 1), core) == 64 * replica_ref[0] + iota((64, 512), 0)
    )
    for k in range(3):
        g = jnp.concatenate([own_ref[k], other_ref[k]], axis=0)
        rows = dot(mine, g).astype(bf16)
        whole = dot(back, g).astype(bf16)
        out_ref[k] = stat_decay * stat_ref[k] + (1.0 - stat_decay) * dot(rows, whole, 1, 1)


def final_kernel(ret_ref, slot_ref, w_ref, out_ref):
    slot = slot_ref[...]
    update = jnp.zeros((64, 512), f32)
    for k in range(3):
        pick = onehot(slot == 3 * iota((64, 64), 1) + k)
        update = update + dot(pick, ret_ref[:, 512 * k : 512 * k + 512])
    for t in range(4):
        for half in range(2):
            row = 4 * half + t
            at = LANES * t + 64 * half
            out_ref[:, row, :] = w_ref[:, row, :] - update[:, at : at + 64]


def slot_table(owners, capacity):
    count = owners.shape[0]
    index = jnp.arange(count, dtype=jnp.int32)
    earlier = (owners[:, None] == owners[None, :]) & (index[None, :] < index[:, None])
    rank = jnp.sum(earlier.astype(jnp.int32), axis=1)
    return owners * capacity + rank


def exchange(x, axis):
    return lax.all_to_all(x, axis, split_axis=0, concat_axis=0, tiled=True)


def local(
    grad_parts,
    weights,
    left_stat,
    right_stat,
    left_codes,
    right_codes,
    left_scales,
    right_scales,
    owners,
):
    core = lax.axis_index("core").astype(jnp.int32)
    replica = (2 * lax.axis_index("x") + core).astype(jnp.int32)[None]
    core = core[None]
    slot_of = slot_table(owners, 3)

    pieces = split(grad_parts.reshape(512, 512))
    left_factor = (left_codes.astype(f32) * left_scales[:, :, None]).astype(bf16)
    right_factor = (right_codes.astype(f32) * right_scales[:, :, None]).astype(bf16)
    left = call(
        left_kernel, [SMEM, *vmem(1), ANY], sds((3, 512, 512), bf16), (core, left_factor, pieces)
    )
    parts = exchange(pieces.reshape(8, 256, 128), ("x", "core"))
    routed = call(
        route_kernel,
        [*vmem(2), ANY],
        sds((64, 1536), bf16),
        (parts, slot_of.reshape(1, 64), left),
    )
    arrived = exchange(routed.reshape(64, 2, 768), "fsdp").reshape(64, 1536)
    own = exchange(call(spread_kernel, vmem(1), sds((4, 768, 128), bf16), (arrived,)), "x")
    other = lax.ppermute(own, "core", [(0, 1), (1, 0)])
    half_grad = sds((3, 256, 512), bf16)
    small = sds((8, 128), f32)
    own_grad, own_pre, own_squares = call(
        own_kernel,
        vmem(3),
        [half_grad, sds((3, 256, 128), f32), small],
        (own, right_factor, left),
    )
    other_grad, pre, squares, grad_squares = call(
        other_kernel,
        vmem(5),
        [half_grad, sds((64, 1536), f32), small, small],
        (other, right_factor, left, own_pre, own_squares),
    )
    all_squares = exchange(squares.reshape(8, 1, 128), ("x", "core")).reshape(8, 128)
    right_new = call(
        right_kernel,
        [SMEM, *vmem(3)],
        sds((3, 64, 512), f32),
        (replica, own_grad, other_grad, right_stat),
    )
    scaled = call(
        scale_kernel, vmem(3), sds((64, 1536), bf16), (all_squares, grad_squares, pre)
    )
    returned = exchange(scaled.reshape(64, 2, 768), "fsdp").reshape(64, 1536)
    left_new = call(
        gram_left_kernel,
        [SMEM, SMEM, *vmem(3), ANY],
        sds((3, 64, 512), f32),
        (replica, core, own_grad, other_grad, left_stat, scaled),
    )
    new_weights = call(
        final_kernel,
        vmem(3),
        sds((64, 8, 64), f32),
        (returned, slot_of.reshape(64, 1), weights),
    )
    return (new_weights, left_new, right_new)


def solution(mesh):
    grid = Mesh(mesh.devices.reshape(64, 4, 2), ("fsdp", "x", "core"))
    dp = ("x", "core")
    return jax.shard_map(
        local,
        mesh=grid,
        in_specs=(
            P(dp, None, "fsdp", None),
            P(None, "fsdp", dp),
            P("fsdp", dp, None),
            P("fsdp", dp, None),
            P("fsdp", None, None),
            P("fsdp", dp, None),
            P("fsdp", None),
            P("fsdp", dp),
            P(),
        ),
        out_specs=(P(None, "fsdp", dp), P("fsdp", dp, None), P("fsdp", dp, None)),
        check_vma=False,
    )
```

```python
import jax
import jax.numpy as jnp
from jax import lax
from jax.experimental import pallas as pl
from jax.experimental.pallas import tpu as pltpu
from jax.sharding import Mesh
from jax.sharding import PartitionSpec as P

stat_decay = 0.95
step_size = 0.5
epsilon = 1e-06

bf16 = jnp.bfloat16
f32 = jnp.float32
LANES = 128
VMEM_GRANT = 16 * 1024 * 1024


def iota(shape, dim):
    return lax.broadcasted_iota(jnp.int32, shape, dim)


def dot(a, b, ca=1, cb=0):
    return lax.dot_general(a, b, (((ca,), (cb,)), ((), ())), preferred_element_type=f32)


def onehot(mask):
    return jnp.where(mask, 1.0, 0.0).astype(bf16)


def natural_row(order, first_half):
    half = (order // 256 + first_half) % 2
    return 8 * (order % 64) + 4 * half + (order // 64) % 4


def vmem(n):
    return [pl.BlockSpec(memory_space=pltpu.VMEM)] * n


SMEM = pl.BlockSpec(memory_space=pltpu.SMEM)
ANY = pl.BlockSpec(memory_space=pl.ANY)


def call(kernel, ins, outs, args):
    single = not isinstance(outs, (list, tuple))
    shapes = [outs] if single else list(outs)
    got = pl.pallas_call(
        kernel,
        out_shape=shapes,
        in_specs=ins,
        out_specs=vmem(len(shapes)),
        compiler_params=pltpu.CompilerParams(vmem_limit_bytes=VMEM_GRANT),
    )(*args)
    return got[0] if single else got


def sds(shape, dtype):
    return jax.ShapeDtypeStruct(shape, dtype)


CHUNKS = 4


def split_kernel(x_ref, out_ref, x_buf, out_buf, in_sem, out_sem):
    rows = x_buf.shape[1]
    per = rows // 8

    def arrival(i):
        return pltpu.make_async_copy(x_ref.at[pl.ds(rows * i, rows)], x_buf.at[i], in_sem.at[i])

    def leaving(i):
        target = out_ref.at[:, :, pl.ds(per * i, per)]
        return pltpu.make_async_copy(out_buf.at[i], target, out_sem.at[i])

    for i in range(CHUNKS):
        arrival(i).start()
    order = iota((rows, rows), 0)
    half, r, block = order // (4 * per), (order // per) % 4, order % per
    perm = onehot(8 * block + 4 * half + r == iota((rows, rows), 1))
    for i in range(CHUNKS):
        arrival(i).wait()
        moved = dot(perm, x_buf[i]).astype(bf16)
        for x in range(4):
            for c in range(2):
                for r in range(4):
                    at = (4 * c + r) * per
                    piece = moved[at : at + per, LANES * x : LANES * x + LANES]
                    out_buf[i, 2 * x + c, r] = piece
        leaving(i).start()
    for i in range(CHUNKS):
        leaving(i).wait()


def split(x):
    rows = 512 // CHUNKS
    return pl.pallas_call(
        split_kernel,
        out_shape=sds((8, 4, 64, 128), bf16),
        in_specs=[ANY],
        out_specs=ANY,
        scratch_shapes=[
            pltpu.VMEM((CHUNKS, rows, 512), bf16),
            pltpu.VMEM((CHUNKS, 8, 4, rows // 8, 128), bf16),
            pltpu.SemaphoreType.DMA((CHUNKS,)),
            pltpu.SemaphoreType.DMA((CHUNKS,)),
        ],
    )(x)


def route_kernel(parts_ref, slot_ref, after_ref, out_ref):
    total = parts_ref[0].astype(f32)
    for s in range(1, 8):
        total = total + parts_ref[s].astype(f32)
    total = total.astype(bf16)
    wide = jnp.concatenate([total[64 * r : 64 * r + 64] for r in range(4)], axis=1)
    slot = slot_ref[...]
    for k in range(3):
        pick = onehot(slot == 3 * iota((64, 64), 0) + k)
        out_ref[:, 512 * k : 512 * k + 512] = dot(pick, wide).astype(bf16)


def left_kernel(core_ref, lc_ref, ls_ref, rc_ref, rs_ref, out_ref, rf_ref):
    back = onehot(natural_row(iota((512, 512), 0), 0) == iota((512, 512), 1))
    cols = onehot(natural_row(iota((512, 512), 1), core_ref[0]) == iota((512, 512), 0))
    for k in range(3):
        factor = (lc_ref[k].astype(f32) * ls_ref[:, k : k + 1]).astype(bf16)
        rows = dot(back, factor).astype(bf16)
        out_ref[k] = dot(rows, cols).astype(bf16)
        rf_ref[k] = (rc_ref[k].astype(f32) * rs_ref[:, k : k + 1]).astype(bf16)


def spread_kernel(piece_ref, out_ref):
    for q in range(4):
        for kr in range(12):
            tile = piece_ref[16 * q : 16 * q + 16, LANES * kr : LANES * kr + LANES]
            for x in range(4):
                at = 192 * q + 16 * kr
                out_ref[x, at : at + 16] = tile


def half_products(at, src_ref, rf_ref, left_ref, g_ref):
    lane = iota((8, LANES), 1)
    grad_squares = jnp.zeros((8, LANES), f32)
    products = []
    for k in range(3):
        for x in range(4):
            for q in range(4):
                for r in range(4):
                    row = 64 * r + 16 * q
                    g_ref[k, row : row + 16, LANES * x : LANES * x + LANES] = src_ref[
                        x, pl.ds(192 * q + 16 * (4 * k + r), 16)
                    ]
        g = g_ref[k]
        rf = rf_ref[k]
        wide = jnp.concatenate([rf, jnp.zeros((128, 512), bf16), rf], axis=0)
        mixed = dot(g, wide, 1, 1).astype(bf16)
        pre = dot(left_ref[k, :256, at : at + 256], mixed[:, :128])
        products.append(pre + dot(left_ref[k, 256:, at : at + 256], mixed[:, 128:]))
        gf = g.astype(f32)
        grad_squares = jnp.where(lane == k, jnp.sum(gf * gf), grad_squares)
    return products, grad_squares


def own_kernel(own_ref, rf_ref, left_ref, g_ref, p_ref, gs_ref):
    products, grad_squares = half_products(0, own_ref, rf_ref, left_ref, g_ref)
    for k in range(3):
        p_ref[k] = products[k]
    gs_ref[...] = grad_squares


def other_kernel(
    other_ref, rf_ref, left_ref, own_p_ref, own_gs_ref, g_ref, p_ref, sq_ref, gs_ref
):
    products, grad_squares = half_products(256, other_ref, rf_ref, left_ref, g_ref)
    lane = iota((8, LANES), 1)
    squares = jnp.zeros((8, LANES), f32)
    for k in range(3):
        pre = own_p_ref[k] + products[k]
        for t in range(4):
            at = 512 * k + LANES * t
            p_ref[:, at : at + LANES] = pre[64 * t : 64 * t + 64]
        squares = jnp.where(lane == k, jnp.sum(pre * pre), squares)
    sq_ref[...] = squares
    gs_ref[...] = own_gs_ref[...] + grad_squares


def scale_kernel(sq_ref, gs_ref, p_ref, out_ref):
    total = jnp.sum(sq_ref[...], axis=0, keepdims=True)
    ratio = step_size * jnp.sqrt(gs_ref[0:1, :]) * lax.rsqrt(total + epsilon)
    for k in range(3):
        span = slice(512 * k, 512 * k + 512)
        out_ref[:, span] = (p_ref[:, span] * ratio[:, k : k + 1]).astype(bf16)


def right_kernel(replica_ref, own_ref, other_ref, stat_ref, out_ref):
    pick = onehot(iota((64, 512), 1) == 64 * replica_ref[0] + iota((64, 512), 0))
    for k in range(3):
        g = jnp.concatenate([own_ref[k], other_ref[k]], axis=0)
        cols = dot(pick, g, 1, 1).astype(bf16)
        out_ref[k] = stat_decay * stat_ref[k] + (1.0 - stat_decay) * dot(cols, g)


def gram_left_kernel(
    replica_ref, core_ref, own_ref, other_ref, stat_ref, after_ref, out_ref
):
    core = core_ref[0]
    order = natural_row(iota((512, 512), 1), core)
    back = onehot(order == iota((512, 512), 0))
    mine = onehot(
        natural_row(iota((64, 512), 1), core) == 64 * replica_ref[0] + iota((64, 512), 0)
    )
    for k in range(3):
        g = jnp.concatenate([own_ref[k], other_ref[k]], axis=0)
        rows = dot(mine, g).astype(bf16)
        whole = dot(back, g).astype(bf16)
        out_ref[k] = stat_decay * stat_ref[k] + (1.0 - stat_decay) * dot(rows, whole, 1, 1)


def final_kernel(ret_ref, slot_ref, w_ref, out_ref, buf, sem):
    slot = slot_ref[...]
    update = jnp.zeros((64, 512), f32)
    for k in range(3):
        pick = onehot(slot == 3 * iota((64, 64), 1) + k)
        update = update + dot(pick, ret_ref[:, 512 * k : 512 * k + 512])
    per = 64 // CHUNKS

    def leaving(i):
        part = pl.ds(per * i, per)
        return pltpu.make_async_copy(buf.at[part], out_ref.at[part], sem.at[i])

    for i in range(CHUNKS):
        part = slice(per * i, per * i + per)
        for t in range(4):
            for half in range(2):
                row = 4 * half + t
                at = LANES * t + 64 * half
                buf[part, row, :] = w_ref[part, row, :] - update[part, at : at + 64]
        leaving(i).start()
    for i in range(CHUNKS):
        leaving(i).wait()


def slot_table(owners, capacity):
    count = owners.shape[0]
    index = jnp.arange(count, dtype=jnp.int32)
    earlier = (owners[:, None] == owners[None, :]) & (index[None, :] < index[:, None])
    rank = jnp.sum(earlier.astype(jnp.int32), axis=1)
    return owners * capacity + rank


def exchange(x, axis):
    return lax.all_to_all(x, axis, split_axis=0, concat_axis=0, tiled=True)


def local(
    grad_parts,
    weights,
    left_stat,
    right_stat,
    left_codes,
    right_codes,
    left_scales,
    right_scales,
    owners,
):
    core = lax.axis_index("core").astype(jnp.int32)
    replica = (2 * lax.axis_index("x") + core).astype(jnp.int32)[None]
    core = core[None]
    slot_of = slot_table(owners, 3)

    pieces = split(grad_parts.reshape(512, 512))
    left, right_factor = call(
        left_kernel,
        [SMEM, *vmem(4)],
        [sds((3, 512, 512), bf16), sds((3, 64, 512), bf16)],
        (core, left_codes, left_scales.T, right_codes, right_scales.T),
    )
    parts = exchange(pieces.reshape(8, 256, 128), ("x", "core"))
    routed = call(
        route_kernel,
        [*vmem(2), ANY],
        sds((64, 1536), bf16),
        (parts, slot_of.reshape(1, 64), left),
    )
    arrived = exchange(routed.reshape(64, 2, 768), "fsdp").reshape(64, 1536)
    own = exchange(call(spread_kernel, vmem(1), sds((4, 768, 128), bf16), (arrived,)), "x")
    other = lax.ppermute(own, "core", [(0, 1), (1, 0)])
    half_grad = sds((3, 256, 512), bf16)
    small = sds((8, 128), f32)
    own_grad, own_pre, own_squares = call(
        own_kernel,
        vmem(3),
        [half_grad, sds((3, 256, 128), f32), small],
        (own, right_factor, left),
    )
    other_grad, pre, squares, grad_squares = call(
        other_kernel,
        vmem(5),
        [half_grad, sds((64, 1536), f32), small, small],
        (other, right_factor, left, own_pre, own_squares),
    )
    all_squares = exchange(squares.reshape(8, 1, 128), ("x", "core")).reshape(8, 128)
    right_new = call(
        right_kernel,
        [SMEM, *vmem(3)],
        sds((3, 64, 512), f32),
        (replica, own_grad, other_grad, right_stat),
    )
    scaled = call(
        scale_kernel, vmem(3), sds((64, 1536), bf16), (all_squares, grad_squares, pre)
    )
    returned = exchange(scaled.reshape(64, 2, 768), "fsdp").reshape(64, 1536)
    left_new = call(
        gram_left_kernel,
        [SMEM, SMEM, *vmem(3), ANY],
        sds((3, 64, 512), f32),
        (replica, core, own_grad, other_grad, left_stat, scaled),
    )
    new_weights = pl.pallas_call(
        final_kernel,
        out_shape=sds((64, 8, 64), f32),
        in_specs=vmem(3),
        out_specs=ANY,
        scratch_shapes=[pltpu.VMEM((64, 8, 64), f32), pltpu.SemaphoreType.DMA((CHUNKS,))],
        compiler_params=pltpu.CompilerParams(vmem_limit_bytes=VMEM_GRANT),
    )(returned, slot_of.reshape(64, 1), weights)
    return (new_weights, left_new, right_new)


def solution(mesh):
    grid = Mesh(mesh.devices.reshape(64, 4, 2), ("fsdp", "x", "core"))
    dp = ("x", "core")
    return jax.shard_map(
        local,
        mesh=grid,
        in_specs=(
            P(dp, None, "fsdp", None),
            P(None, "fsdp", dp),
            P("fsdp", dp, None),
            P("fsdp", dp, None),
            P("fsdp", None, None),
            P("fsdp", dp, None),
            P("fsdp", None),
            P("fsdp", dp),
            P(),
        ),
        out_specs=(P(None, "fsdp", dp), P("fsdp", dp, None), P("fsdp", dp, None)),
        check_vma=False,
    )
```

```python
import jax
import jax.numpy as jnp
from jax import lax
from jax.experimental import pallas as pl
from jax.experimental.pallas import tpu as pltpu
from jax.sharding import Mesh
from jax.sharding import PartitionSpec as P

stat_decay = 0.95
step_size = 0.5
epsilon = 1e-06

bf16 = jnp.bfloat16
f32 = jnp.float32
LANES = 128
VMEM_GRANT = 16 * 1024 * 1024


def iota(shape, dim):
    return lax.broadcasted_iota(jnp.int32, shape, dim)


def dot(a, b, ca=1, cb=0):
    return lax.dot_general(a, b, (((ca,), (cb,)), ((), ())), preferred_element_type=f32)


def onehot(mask):
    return jnp.where(mask, 1.0, 0.0).astype(bf16)


def natural_row(order, first_half):
    half = (order // 256 + first_half) % 2
    return 8 * (order % 64) + 4 * half + (order // 64) % 4


def vmem(n):
    return [pl.BlockSpec(memory_space=pltpu.VMEM)] * n


SMEM = pl.BlockSpec(memory_space=pltpu.SMEM)
ANY = pl.BlockSpec(memory_space=pl.ANY)


def call(kernel, ins, outs, args):
    single = not isinstance(outs, (list, tuple))
    shapes = [outs] if single else list(outs)
    got = pl.pallas_call(
        kernel,
        out_shape=shapes,
        in_specs=ins,
        out_specs=vmem(len(shapes)),
        compiler_params=pltpu.CompilerParams(vmem_limit_bytes=VMEM_GRANT),
    )(*args)
    return got[0] if single else got


def sds(shape, dtype):
    return jax.ShapeDtypeStruct(shape, dtype)


CHUNKS = 4


def split_kernel(x_ref, out_ref, buf, sem):
    rows = 512 // CHUNKS
    per = rows // 8

    def leaving(i):
        return pltpu.make_async_copy(buf.at[i], out_ref.at[:, :, pl.ds(per * i, per)], sem.at[i])

    order = iota((rows, rows), 0)
    half, r, block = order // (4 * per), (order // per) % 4, order % per
    perm = onehot(8 * block + 4 * half + r == iota((rows, rows), 1))
    for i in range(CHUNKS):
        moved = dot(perm, x_ref[rows * i : rows * i + rows]).astype(bf16)
        for x in range(4):
            for c in range(2):
                for r in range(4):
                    at = (4 * c + r) * per
                    piece = moved[at : at + per, LANES * x : LANES * x + LANES]
                    buf[i, 2 * x + c, r] = piece
        leaving(i).start()
    for i in range(CHUNKS):
        leaving(i).wait()


def split(x):
    return pl.pallas_call(
        split_kernel,
        out_shape=sds((8, 4, 64, 128), bf16),
        in_specs=vmem(1),
        out_specs=ANY,
        scratch_shapes=[
            pltpu.VMEM((CHUNKS, 8, 4, 64 // CHUNKS, 128), bf16),
            pltpu.SemaphoreType.DMA((CHUNKS,)),
        ],
        compiler_params=pltpu.CompilerParams(vmem_limit_bytes=VMEM_GRANT),
    )(x)


def route_kernel(parts_ref, slot_ref, out_ref):
    total = parts_ref[0].astype(f32)
    for s in range(1, 8):
        total = total + parts_ref[s].astype(f32)
    total = total.astype(bf16)
    wide = jnp.concatenate([total[64 * r : 64 * r + 64] for r in range(4)], axis=1)
    slot = slot_ref[...]
    for k in range(3):
        pick = onehot(slot == 3 * iota((64, 64), 0) + k)
        out_ref[:, 512 * k : 512 * k + 512] = dot(pick, wide).astype(bf16)


def left_kernel(core_ref, lc_ref, ls_ref, rc_ref, rs_ref, after_ref, out_ref, rf_ref):
    back = onehot(natural_row(iota((512, 512), 0), 0) == iota((512, 512), 1))
    cols = onehot(natural_row(iota((512, 512), 1), core_ref[0]) == iota((512, 512), 0))
    for k in range(3):
        factor = (lc_ref[k].astype(f32) * ls_ref[:, k : k + 1]).astype(bf16)
        rows = dot(back, factor).astype(bf16)
        out_ref[k] = dot(rows, cols).astype(bf16)
        rf_ref[k] = (rc_ref[k].astype(f32) * rs_ref[:, k : k + 1]).astype(bf16)


def spread_kernel(piece_ref, after_ref, out_ref):
    for q in range(4):
        for kr in range(12):
            tile = piece_ref[16 * q : 16 * q + 16, LANES * kr : LANES * kr + LANES]
            for x in range(4):
                at = 192 * q + 16 * kr
                out_ref[x, at : at + 16] = tile


def half_products(at, src_ref, rf_ref, left_ref, g_ref):
    lane = iota((8, LANES), 1)
    grad_squares = jnp.zeros((8, LANES), f32)
    products = []
    for k in range(3):
        for x in range(4):
            for q in range(4):
                for r in range(4):
                    row = 64 * r + 16 * q
                    g_ref[k, row : row + 16, LANES * x : LANES * x + LANES] = src_ref[
                        x, pl.ds(192 * q + 16 * (4 * k + r), 16)
                    ]
        g = g_ref[k]
        rf = rf_ref[k]
        wide = jnp.concatenate([rf, jnp.zeros((128, 512), bf16), rf], axis=0)
        mixed = dot(g, wide, 1, 1).astype(bf16)
        pre = dot(left_ref[k, :256, at : at + 256], mixed[:, :128])
        products.append(pre + dot(left_ref[k, 256:, at : at + 256], mixed[:, 128:]))
        gf = g.astype(f32)
        grad_squares = jnp.where(lane == k, jnp.sum(gf * gf), grad_squares)
    return products, grad_squares


def own_kernel(own_ref, rf_ref, left_ref, g_ref, p_ref, gs_ref):
    products, grad_squares = half_products(0, own_ref, rf_ref, left_ref, g_ref)
    for k in range(3):
        p_ref[k] = products[k]
    gs_ref[...] = grad_squares


def other_kernel(
    other_ref, rf_ref, left_ref, own_p_ref, own_gs_ref, g_ref, p_ref, sq_ref, gs_ref
):
    products, grad_squares = half_products(256, other_ref, rf_ref, left_ref, g_ref)
    lane = iota((8, LANES), 1)
    squares = jnp.zeros((8, LANES), f32)
    for k in range(3):
        pre = own_p_ref[k] + products[k]
        for t in range(4):
            at = 512 * k + LANES * t
            p_ref[:, at : at + LANES] = pre[64 * t : 64 * t + 64]
        squares = jnp.where(lane == k, jnp.sum(pre * pre), squares)
    sq_ref[...] = squares
    gs_ref[...] = own_gs_ref[...] + grad_squares


def scale_kernel(sq_ref, gs_ref, p_ref, out_ref):
    total = jnp.sum(sq_ref[...], axis=0, keepdims=True)
    ratio = step_size * jnp.sqrt(gs_ref[0:1, :]) * lax.rsqrt(total + epsilon)
    for k in range(3):
        span = slice(512 * k, 512 * k + 512)
        out_ref[:, span] = (p_ref[:, span] * ratio[:, k : k + 1]).astype(bf16)


def right_kernel(replica_ref, own_ref, other_ref, stat_ref, out_ref):
    pick = onehot(iota((64, 512), 1) == 64 * replica_ref[0] + iota((64, 512), 0))
    for k in range(3):
        g = jnp.concatenate([own_ref[k], other_ref[k]], axis=0)
        cols = dot(pick, g, 1, 1).astype(bf16)
        out_ref[k] = stat_decay * stat_ref[k] + (1.0 - stat_decay) * dot(cols, g)


def gram_left_kernel(
    replica_ref, core_ref, own_ref, other_ref, stat_ref, after_ref, out_ref
):
    core = core_ref[0]
    order = natural_row(iota((512, 512), 1), core)
    back = onehot(order == iota((512, 512), 0))
    mine = onehot(
        natural_row(iota((64, 512), 1), core) == 64 * replica_ref[0] + iota((64, 512), 0)
    )
    for k in range(3):
        g = jnp.concatenate([own_ref[k], other_ref[k]], axis=0)
        rows = dot(mine, g).astype(bf16)
        whole = dot(back, g).astype(bf16)
        out_ref[k] = stat_decay * stat_ref[k] + (1.0 - stat_decay) * dot(rows, whole, 1, 1)


def final_kernel(ret_ref, slot_ref, w_ref, out_ref, buf, sem):
    slot = slot_ref[...]
    update = jnp.zeros((64, 512), f32)
    for k in range(3):
        pick = onehot(slot == 3 * iota((64, 64), 1) + k)
        update = update + dot(pick, ret_ref[:, 512 * k : 512 * k + 512])
    per = 64 // CHUNKS

    def leaving(i):
        part = pl.ds(per * i, per)
        return pltpu.make_async_copy(buf.at[part], out_ref.at[part], sem.at[i])

    for i in range(CHUNKS):
        part = slice(per * i, per * i + per)
        for t in range(4):
            for half in range(2):
                row = 4 * half + t
                at = LANES * t + 64 * half
                buf[part, row, :] = w_ref[part, row, :] - update[part, at : at + 64]
        leaving(i).start()
    for i in range(CHUNKS):
        leaving(i).wait()


def slot_table(owners, capacity):
    count = owners.shape[0]
    index = jnp.arange(count, dtype=jnp.int32)
    earlier = (owners[:, None] == owners[None, :]) & (index[None, :] < index[:, None])
    rank = jnp.sum(earlier.astype(jnp.int32), axis=1)
    return owners * capacity + rank


def exchange(x, axis):
    return lax.all_to_all(x, axis, split_axis=0, concat_axis=0, tiled=True)


def local(
    grad_parts,
    weights,
    left_stat,
    right_stat,
    left_codes,
    right_codes,
    left_scales,
    right_scales,
    owners,
):
    core = lax.axis_index("core").astype(jnp.int32)
    replica = (2 * lax.axis_index("x") + core).astype(jnp.int32)[None]
    core = core[None]
    slot_of = slot_table(owners, 3)

    pieces = split(grad_parts.reshape(512, 512))
    parts = exchange(pieces.reshape(8, 256, 128), ("x", "core"))
    routed = call(
        route_kernel, vmem(2), sds((64, 1536), bf16), (parts, slot_of.reshape(1, 64))
    )
    left, right_factor = call(
        left_kernel,
        [SMEM, *vmem(4), ANY],
        [sds((3, 512, 512), bf16), sds((3, 64, 512), bf16)],
        (core, left_codes, left_scales.T, right_codes, right_scales.T, routed),
    )
    arrived = exchange(routed.reshape(64, 2, 768), "fsdp").reshape(64, 1536)
    spread = call(
        spread_kernel, [*vmem(1), ANY], sds((4, 768, 128), bf16), (arrived, right_factor)
    )
    own = exchange(spread, "x")
    other = lax.ppermute(own, "core", [(0, 1), (1, 0)])
    half_grad = sds((3, 256, 512), bf16)
    small = sds((8, 128), f32)
    own_grad, own_pre, own_squares = call(
        own_kernel,
        vmem(3),
        [half_grad, sds((3, 256, 128), f32), small],
        (own, right_factor, left),
    )
    other_grad, pre, squares, grad_squares = call(
        other_kernel,
        vmem(5),
        [half_grad, sds((64, 1536), f32), small, small],
        (other, right_factor, left, own_pre, own_squares),
    )
    all_squares = exchange(squares.reshape(8, 1, 128), ("x", "core")).reshape(8, 128)
    right_new = call(
        right_kernel,
        [SMEM, *vmem(3)],
        sds((3, 64, 512), f32),
        (replica, own_grad, other_grad, right_stat),
    )
    scaled = call(
        scale_kernel, vmem(3), sds((64, 1536), bf16), (all_squares, grad_squares, pre)
    )
    returned = exchange(scaled.reshape(64, 2, 768), "fsdp").reshape(64, 1536)
    left_new = call(
        gram_left_kernel,
        [SMEM, SMEM, *vmem(3), ANY],
        sds((3, 64, 512), f32),
        (replica, core, own_grad, other_grad, left_stat, scaled),
    )
    new_weights = pl.pallas_call(
        final_kernel,
        out_shape=sds((64, 8, 64), f32),
        in_specs=vmem(3),
        out_specs=ANY,
        scratch_shapes=[pltpu.VMEM((64, 8, 64), f32), pltpu.SemaphoreType.DMA((CHUNKS,))],
        compiler_params=pltpu.CompilerParams(vmem_limit_bytes=VMEM_GRANT),
    )(returned, slot_of.reshape(64, 1), weights)
    return (new_weights, left_new, right_new)


def solution(mesh):
    grid = Mesh(mesh.devices.reshape(64, 4, 2), ("fsdp", "x", "core"))
    dp = ("x", "core")
    return jax.shard_map(
        local,
        mesh=grid,
        in_specs=(
            P(dp, None, "fsdp", None),
            P(None, "fsdp", dp),
            P("fsdp", dp, None),
            P("fsdp", dp, None),
            P("fsdp", None, None),
            P("fsdp", dp, None),
            P("fsdp", None),
            P("fsdp", dp),
            P(),
        ),
        out_specs=(P(None, "fsdp", dp), P("fsdp", dp, None), P("fsdp", dp, None)),
        check_vma=False,
    )
```

```python
import jax
import jax.numpy as jnp
from jax import lax
from jax.experimental import pallas as pl
from jax.experimental.pallas import tpu as pltpu
from jax.sharding import Mesh
from jax.sharding import PartitionSpec as P

stat_decay = 0.95
step_size = 0.5
epsilon = 1e-06

bf16 = jnp.bfloat16
f32 = jnp.float32
LANES = 128
VMEM_GRANT = 16 * 1024 * 1024


def iota(shape, dim):
    return lax.broadcasted_iota(jnp.int32, shape, dim)


def dot(a, b, ca=1, cb=0):
    return lax.dot_general(a, b, (((ca,), (cb,)), ((), ())), preferred_element_type=f32)


def onehot(mask):
    return jnp.where(mask, 1.0, 0.0).astype(bf16)


def natural_row(order, first_half):
    half = (order // 256 + first_half) % 2
    return 8 * (order % 64) + 4 * half + (order // 64) % 4


def vmem(n):
    return [pl.BlockSpec(memory_space=pltpu.VMEM)] * n


SMEM = pl.BlockSpec(memory_space=pltpu.SMEM)
ANY = pl.BlockSpec(memory_space=pl.ANY)


def call(kernel, ins, outs, args):
    single = not isinstance(outs, (list, tuple))
    shapes = [outs] if single else list(outs)
    got = pl.pallas_call(
        kernel,
        out_shape=shapes,
        in_specs=ins,
        out_specs=vmem(len(shapes)),
        compiler_params=pltpu.CompilerParams(vmem_limit_bytes=VMEM_GRANT),
    )(*args)
    return got[0] if single else got


def sds(shape, dtype):
    return jax.ShapeDtypeStruct(shape, dtype)


CHUNKS = 4


def split_kernel(x_ref, out_ref, buf, sem):
    rows = 512 // CHUNKS
    per = rows // 8

    def leaving(i):
        return pltpu.make_async_copy(buf.at[i], out_ref.at[:, :, pl.ds(per * i, per)], sem.at[i])

    order = iota((rows, rows), 0)
    half, r, block = order // (4 * per), (order // per) % 4, order % per
    perm = onehot(8 * block + 4 * half + r == iota((rows, rows), 1))
    for i in range(CHUNKS):
        moved = dot(perm, x_ref[rows * i : rows * i + rows]).astype(bf16)
        for x in range(4):
            for c in range(2):
                for r in range(4):
                    at = (4 * c + r) * per
                    piece = moved[at : at + per, LANES * x : LANES * x + LANES]
                    buf[i, 2 * x + c, r] = piece
        leaving(i).start()
    for i in range(CHUNKS):
        leaving(i).wait()


def split(x):
    return pl.pallas_call(
        split_kernel,
        out_shape=sds((8, 4, 64, 128), bf16),
        in_specs=vmem(1),
        out_specs=ANY,
        scratch_shapes=[
            pltpu.VMEM((CHUNKS, 8, 4, 64 // CHUNKS, 128), bf16),
            pltpu.SemaphoreType.DMA((CHUNKS,)),
        ],
        compiler_params=pltpu.CompilerParams(vmem_limit_bytes=VMEM_GRANT),
    )(x)


def route_kernel(parts_ref, slot_ref, after_ref, out_ref):
    total = parts_ref[0].astype(f32)
    for s in range(1, 8):
        total = total + parts_ref[s].astype(f32)
    total = total.astype(bf16)
    wide = jnp.concatenate([total[64 * r : 64 * r + 64] for r in range(4)], axis=1)
    slot = slot_ref[...]
    for k in range(3):
        pick = onehot(slot == 3 * iota((64, 64), 0) + k)
        out_ref[:, 512 * k : 512 * k + 512] = dot(pick, wide).astype(bf16)


def left_kernel(core_ref, lc_ref, ls_ref, rc_ref, rs_ref, out_ref, rf_ref):
    back = onehot(natural_row(iota((512, 512), 0), 0) == iota((512, 512), 1))
    cols = onehot(natural_row(iota((512, 512), 1), core_ref[0]) == iota((512, 512), 0))
    for k in range(3):
        factor = (lc_ref[k].astype(f32) * ls_ref[:, k : k + 1]).astype(bf16)
        rows = dot(back, factor).astype(bf16)
        out_ref[k] = dot(rows, cols).astype(bf16)
        rf_ref[k] = (rc_ref[k].astype(f32) * rs_ref[:, k : k + 1]).astype(bf16)


def spread_kernel(piece_ref, f0_ref, f1_ref, f2_ref, f3_ref, out_ref, near_ref):
    for x, ref in enumerate((f0_ref, f1_ref, f2_ref, f3_ref)):
        near_ref[x] = ref[...]
    for q in range(4):
        for kr in range(12):
            tile = piece_ref[16 * q : 16 * q + 16, LANES * kr : LANES * kr + LANES]
            for x in range(4):
                at = 192 * q + 16 * kr
                out_ref[x, at : at + 16] = tile


def gather_half(k, src_ref, g_ref):
    for x in range(4):
        for q in range(4):
            for r in range(4):
                row = 64 * r + 16 * q
                g_ref[k, row : row + 16, LANES * x : LANES * x + LANES] = src_ref[
                    x, pl.ds(192 * q + 16 * (4 * k + r), 16)
                ]


def times_factor(g, factor_ref, k):
    factor = jnp.concatenate([factor_ref[x, k] for x in range(4)], axis=0)
    return dot(g, factor, 1, 1).astype(bf16)


def own_kernel(own_ref, near_ref, g_ref, m_ref, gs_ref):
    lane = iota((8, LANES), 1)
    grad_squares = jnp.zeros((8, LANES), f32)
    for k in range(3):
        gather_half(k, own_ref, g_ref)
        g = g_ref[k]
        m_ref[k] = times_factor(g, near_ref, k)
        gf = g.astype(f32)
        grad_squares = jnp.where(lane == k, jnp.sum(gf * gf), grad_squares)
    gs_ref[...] = grad_squares


def other_kernel(
    other_ref, near_ref, far_ref, left_ref, own_g_ref, own_m_ref, own_gs_ref, g_ref, out_ref
):
    low = iota((256, LANES), 1) < 64
    for k in range(3):
        gather_half(k, other_ref, g_ref)
        g = g_ref[k]
        gf = g.astype(f32)
        squares = own_gs_ref[0:1, k : k + 1] + jnp.sum(gf * gf)
        mixed = jnp.concatenate([own_m_ref[k], times_factor(g, near_ref, k)], axis=0)
        pre = dot(left_ref[k], mixed)
        total = jnp.sum(pre * pre)
        mine = jnp.where(low, pre[:256, :128], pltpu.roll(pre[256:, :128], 64, 1))
        whole = jnp.concatenate([own_g_ref[k], g], axis=0)
        pre = dot(left_ref[k], times_factor(whole, far_ref, k))
        total = total + jnp.sum(pre * pre)
        ratio = step_size * jnp.sqrt(squares) * lax.rsqrt(jnp.full((1, 1), total) + epsilon)
        mine = (mine * ratio).astype(bf16)
        for t in range(4):
            at = 512 * k + LANES * t
            out_ref[:, at : at + LANES] = mine[64 * t : 64 * t + 64]


def right_kernel(replica_ref, own_ref, other_ref, stat_ref, out_ref):
    pick = onehot(iota((64, 512), 1) == 64 * replica_ref[0] + iota((64, 512), 0))
    for k in range(3):
        g = jnp.concatenate([own_ref[k], other_ref[k]], axis=0)
        cols = dot(pick, g, 1, 1).astype(bf16)
        out_ref[k] = stat_decay * stat_ref[k] + (1.0 - stat_decay) * dot(cols, g)


def gram_left_kernel(
    replica_ref, core_ref, own_ref, other_ref, stat_ref, after_ref, out_ref
):
    core = core_ref[0]
    order = natural_row(iota((512, 512), 1), core)
    back = onehot(order == iota((512, 512), 0))
    mine = onehot(
        natural_row(iota((64, 512), 1), core) == 64 * replica_ref[0] + iota((64, 512), 0)
    )
    for k in range(3):
        g = jnp.concatenate([own_ref[k], other_ref[k]], axis=0)
        rows = dot(mine, g).astype(bf16)
        whole = dot(back, g).astype(bf16)
        out_ref[k] = stat_decay * stat_ref[k] + (1.0 - stat_decay) * dot(rows, whole, 1, 1)


def final_kernel(ret_ref, slot_ref, w_ref, out_ref, buf, sem):
    slot = slot_ref[...]
    update = jnp.zeros((64, 512), f32)
    for k in range(3):
        pick = onehot(slot == 3 * iota((64, 64), 1) + k)
        update = update + dot(pick, ret_ref[:, 512 * k : 512 * k + 512])
    per = 64 // CHUNKS

    def leaving(i):
        part = pl.ds(per * i, per)
        return pltpu.make_async_copy(buf.at[part], out_ref.at[part], sem.at[i])

    for i in range(CHUNKS):
        part = slice(per * i, per * i + per)
        for t in range(4):
            for half in range(2):
                row = 4 * half + t
                at = LANES * t + 64 * half
                buf[part, row, :] = w_ref[part, row, :] - update[part, at : at + 64]
        leaving(i).start()
    for i in range(CHUNKS):
        leaving(i).wait()


def slot_table(owners, capacity):
    count = owners.shape[0]
    index = jnp.arange(count, dtype=jnp.int32)
    earlier = (owners[:, None] == owners[None, :]) & (index[None, :] < index[:, None])
    rank = jnp.sum(earlier.astype(jnp.int32), axis=1)
    return owners * capacity + rank


def exchange(x, axis):
    return lax.all_to_all(x, axis, split_axis=0, concat_axis=0, tiled=True)


def local(
    grad_parts,
    weights,
    left_stat,
    right_stat,
    left_codes,
    right_codes,
    left_scales,
    right_scales,
    owners,
):
    core = lax.axis_index("core").astype(jnp.int32)
    replica = (2 * lax.axis_index("x") + core).astype(jnp.int32)[None]
    core = core[None]
    slot_of = slot_table(owners, 3)

    pieces = split(grad_parts.reshape(512, 512))
    left, right_factor = call(
        left_kernel,
        [SMEM, *vmem(4)],
        [sds((3, 512, 512), bf16), sds((3, 64, 512), bf16)],
        (core, left_codes, left_scales.T, right_codes, right_scales.T),
    )
    parts = exchange(pieces.reshape(8, 256, 128), ("x", "core"))
    routed = call(
        route_kernel,
        [*vmem(2), ANY],
        sds((64, 1536), bf16),
        (parts, slot_of.reshape(1, 64), left),
    )
    swap = [(0, 1), (1, 0)]
    arrived = exchange(routed.reshape(64, 2, 768), "fsdp").reshape(64, 1536)
    shared = [right_factor]
    for step in (2, 1, 3):
        ring = [(x, (x + step) % 4) for x in range(4)]
        shared.append(lax.ppermute(right_factor, "x", ring))
    spread, near = call(
        spread_kernel,
        vmem(5),
        [sds((4, 768, 128), bf16), sds((4, 3, 64, 512), bf16)],
        (arrived, *shared),
    )
    own, near = lax.optimization_barrier((exchange(spread, "x"), near))
    far = lax.ppermute(near, "core", swap)
    other = lax.ppermute(own, "core", swap)
    half_grad = sds((3, 256, 512), bf16)
    own_grad, own_mixed, own_squares = call(
        own_kernel,
        vmem(2),
        [half_grad, sds((3, 256, 256), bf16), sds((8, 128), f32)],
        (own, near),
    )
    other_grad, scaled = call(
        other_kernel,
        vmem(7),
        [half_grad, sds((64, 1536), bf16)],
        (other, near, far, left, own_grad, own_mixed, own_squares),
    )
    right_new = call(
        right_kernel,
        [SMEM, *vmem(3)],
        sds((3, 64, 512), f32),
        (replica, own_grad, other_grad, right_stat),
    )
    returned = exchange(scaled.reshape(64, 2, 768), "fsdp").reshape(64, 1536)
    left_new = call(
        gram_left_kernel,
        [SMEM, SMEM, *vmem(3), ANY],
        sds((3, 64, 512), f32),
        (replica, core, own_grad, other_grad, left_stat, scaled),
    )
    new_weights = pl.pallas_call(
        final_kernel,
        out_shape=sds((64, 8, 64), f32),
        in_specs=vmem(3),
        out_specs=ANY,
        scratch_shapes=[pltpu.VMEM((64, 8, 64), f32), pltpu.SemaphoreType.DMA((CHUNKS,))],
        compiler_params=pltpu.CompilerParams(vmem_limit_bytes=VMEM_GRANT),
    )(returned, slot_of.reshape(64, 1), weights)
    return (new_weights, left_new, right_new)


def solution(mesh):
    grid = Mesh(mesh.devices.reshape(64, 4, 2), ("fsdp", "x", "core"))
    dp = ("x", "core")
    return jax.shard_map(
        local,
        mesh=grid,
        in_specs=(
            P(dp, None, "fsdp", None),
            P(None, "fsdp", dp),
            P("fsdp", dp, None),
            P("fsdp", dp, None),
            P("fsdp", None, None),
            P("fsdp", dp, None),
            P("fsdp", None),
            P("fsdp", dp),
            P(),
        ),
        out_specs=(P(None, "fsdp", dp), P("fsdp", dp, None), P("fsdp", dp, None)),
        check_vma=False,
    )
```

```python
import jax
import jax.numpy as jnp
from jax import lax
from jax.experimental import pallas as pl
from jax.experimental.pallas import tpu as pltpu
from jax.sharding import Mesh
from jax.sharding import PartitionSpec as P

stat_decay = 0.95
step_size = 0.5
epsilon = 1e-06

bf16 = jnp.bfloat16
f32 = jnp.float32
LANES = 128
VMEM_GRANT = 16 * 1024 * 1024


def iota(shape, dim):
    return lax.broadcasted_iota(jnp.int32, shape, dim)


def dot(a, b, ca=1, cb=0):
    return lax.dot_general(a, b, (((ca,), (cb,)), ((), ())), preferred_element_type=f32)


def onehot(mask):
    return jnp.where(mask, 1.0, 0.0).astype(bf16)


def natural_row(order, first_half):
    half = (order // 256 + first_half) % 2
    return 8 * (order % 64) + 4 * half + (order // 64) % 4


def vmem(n):
    return [pl.BlockSpec(memory_space=pltpu.VMEM)] * n


SMEM = pl.BlockSpec(memory_space=pltpu.SMEM)
ANY = pl.BlockSpec(memory_space=pl.ANY)


def call(kernel, ins, outs, args):
    single = not isinstance(outs, (list, tuple))
    shapes = [outs] if single else list(outs)
    got = pl.pallas_call(
        kernel,
        out_shape=shapes,
        in_specs=ins,
        out_specs=vmem(len(shapes)),
        compiler_params=pltpu.CompilerParams(vmem_limit_bytes=VMEM_GRANT),
    )(*args)
    return got[0] if single else got


def sds(shape, dtype):
    return jax.ShapeDtypeStruct(shape, dtype)


CHUNKS = 4


def split_kernel(x_ref, out_ref, buf, sem):
    rows = 512 // CHUNKS
    per = rows // 8

    def leaving(i):
        return pltpu.make_async_copy(buf.at[i], out_ref.at[:, :, pl.ds(per * i, per)], sem.at[i])

    order = iota((rows, rows), 0)
    half, r, block = order // (4 * per), (order // per) % 4, order % per
    perm = onehot(8 * block + 4 * half + r == iota((rows, rows), 1))
    for i in range(CHUNKS):
        moved = dot(perm, x_ref[rows * i : rows * i + rows]).astype(bf16)
        for x in range(4):
            for c in range(2):
                for r in range(4):
                    at = (4 * c + r) * per
                    piece = moved[at : at + per, LANES * x : LANES * x + LANES]
                    buf[i, 2 * x + c, r] = piece
        leaving(i).start()
    for i in range(CHUNKS):
        leaving(i).wait()


def split(x):
    return pl.pallas_call(
        split_kernel,
        out_shape=sds((8, 4, 64, 128), bf16),
        in_specs=vmem(1),
        out_specs=ANY,
        scratch_shapes=[
            pltpu.VMEM((CHUNKS, 8, 4, 64 // CHUNKS, 128), bf16),
            pltpu.SemaphoreType.DMA((CHUNKS,)),
        ],
        compiler_params=pltpu.CompilerParams(vmem_limit_bytes=VMEM_GRANT),
    )(x)


def route_kernel(parts_ref, slot_ref, after_ref, out_ref):
    total = parts_ref[0].astype(f32)
    for s in range(1, 8):
        total = total + parts_ref[s].astype(f32)
    total = total.astype(bf16)
    wide = jnp.concatenate([total[64 * r : 64 * r + 64] for r in range(4)], axis=1)
    slot = slot_ref[...]
    for k in range(3):
        pick = onehot(slot == 3 * iota((64, 64), 0) + k)
        out_ref[:, 512 * k : 512 * k + 512] = dot(pick, wide).astype(bf16)


def left_kernel(core_ref, lc_ref, ls_ref, rc_ref, rs_ref, out_ref, rf_ref):
    back = onehot(natural_row(iota((512, 512), 0), 0) == iota((512, 512), 1))
    cols = onehot(natural_row(iota((512, 512), 1), core_ref[0]) == iota((512, 512), 0))
    for k in range(3):
        factor = (lc_ref[k].astype(f32) * ls_ref[:, k : k + 1]).astype(bf16)
        rows = dot(back, factor).astype(bf16)
        out_ref[k] = dot(rows, cols).astype(bf16)
        rf_ref[k] = (rc_ref[k].astype(f32) * rs_ref[:, k : k + 1]).astype(bf16)


def spread_kernel(piece_ref, out_ref):
    for q in range(4):
        for kr in range(12):
            tile = piece_ref[16 * q : 16 * q + 16, LANES * kr : LANES * kr + LANES]
            for x in range(4):
                at = 192 * q + 16 * kr
                out_ref[x, at : at + 16] = tile


def half_products(at, src_ref, rf_ref, left_ref, g_ref):
    lane = iota((8, LANES), 1)
    grad_squares = jnp.zeros((8, LANES), f32)
    products = []
    for k in range(3):
        for x in range(4):
            for q in range(4):
                for r in range(4):
                    row = 64 * r + 16 * q
                    g_ref[k, row : row + 16, LANES * x : LANES * x + LANES] = src_ref[
                        x, pl.ds(192 * q + 16 * (4 * k + r), 16)
                    ]
        g = g_ref[k]
        rf = rf_ref[k]
        wide = jnp.concatenate([rf, jnp.zeros((128, 512), bf16), rf], axis=0)
        mixed = dot(g, wide, 1, 1).astype(bf16)
        pre = dot(left_ref[k, :256, at : at + 256], mixed[:, :128])
        products.append(pre + dot(left_ref[k, 256:, at : at + 256], mixed[:, 128:]))
        gf = g.astype(f32)
        grad_squares = jnp.where(lane == k, jnp.sum(gf * gf), grad_squares)
    return products, grad_squares


def own_kernel(own_ref, rf_ref, left_ref, g_ref, p_ref, gs_ref):
    products, grad_squares = half_products(0, own_ref, rf_ref, left_ref, g_ref)
    for k in range(3):
        p_ref[k] = products[k]
    gs_ref[...] = grad_squares


def other_kernel(
    other_ref, rf_ref, left_ref, own_p_ref, own_gs_ref, g_ref, p_ref, sq_ref, gs_ref
):
    products, grad_squares = half_products(256, other_ref, rf_ref, left_ref, g_ref)
    lane = iota((8, LANES), 1)
    squares = jnp.zeros((8, LANES), f32)
    for k in range(3):
        pre = own_p_ref[k] + products[k]
        for t in range(4):
            at = 512 * k + LANES * t
            p_ref[:, at : at + LANES] = pre[64 * t : 64 * t + 64]
        squares = jnp.where(lane == k, jnp.sum(pre * pre), squares)
    sq_ref[...] = squares
    gs_ref[...] = own_gs_ref[...] + grad_squares


def scale_kernel(sq_ref, gs_ref, p_ref, out_ref):
    total = jnp.sum(sq_ref[...], axis=0, keepdims=True)
    ratio = step_size * jnp.sqrt(gs_ref[0:1, :]) * lax.rsqrt(total + epsilon)
    for k in range(3):
        span = slice(512 * k, 512 * k + 512)
        out_ref[:, span] = (p_ref[:, span] * ratio[:, k : k + 1]).astype(bf16)


def right_kernel(replica_ref, own_ref, other_ref, stat_ref, out_ref):
    pick = onehot(iota((64, 512), 1) == 64 * replica_ref[0] + iota((64, 512), 0))
    for k in range(3):
        g = jnp.concatenate([own_ref[k], other_ref[k]], axis=0)
        cols = dot(pick, g, 1, 1).astype(bf16)
        out_ref[k] = stat_decay * stat_ref[k] + (1.0 - stat_decay) * dot(cols, g)


def gram_left_kernel(
    replica_ref, core_ref, own_ref, other_ref, stat_ref, after_ref, out_ref
):
    core = core_ref[0]
    order = natural_row(iota((512, 512), 1), core)
    back = onehot(order == iota((512, 512), 0))
    mine = onehot(
        natural_row(iota((64, 512), 1), core) == 64 * replica_ref[0] + iota((64, 512), 0)
    )
    for k in range(3):
        g = jnp.concatenate([own_ref[k], other_ref[k]], axis=0)
        rows = dot(mine, g).astype(bf16)
        whole = dot(back, g).astype(bf16)
        out_ref[k] = stat_decay * stat_ref[k] + (1.0 - stat_decay) * dot(rows, whole, 1, 1)


def final_kernel(ret_ref, slot_ref, w_ref, out_ref, buf, sem):
    slot = slot_ref[...]
    update = jnp.zeros((64, 512), f32)
    for k in range(3):
        pick = onehot(slot == 3 * iota((64, 64), 1) + k)
        update = update + dot(pick, ret_ref[:, 512 * k : 512 * k + 512])
    per = 64 // CHUNKS

    def leaving(i):
        part = pl.ds(per * i, per)
        return pltpu.make_async_copy(buf.at[part], out_ref.at[part], sem.at[i])

    for i in range(CHUNKS):
        part = slice(per * i, per * i + per)
        for t in range(4):
            for half in range(2):
                row = 4 * half + t
                at = LANES * t + 64 * half
                buf[part, row, :] = w_ref[part, row, :] - update[part, at : at + 64]
        leaving(i).start()
    for i in range(CHUNKS):
        leaving(i).wait()


def slot_table(owners, capacity):
    count = owners.shape[0]
    index = jnp.arange(count, dtype=jnp.int32)
    earlier = (owners[:, None] == owners[None, :]) & (index[None, :] < index[:, None])
    rank = jnp.sum(earlier.astype(jnp.int32), axis=1)
    return owners * capacity + rank


def exchange(x, axis):
    return lax.all_to_all(x, axis, split_axis=0, concat_axis=0, tiled=True)


def local(
    grad_parts,
    weights,
    left_stat,
    right_stat,
    left_codes,
    right_codes,
    left_scales,
    right_scales,
    owners,
):
    core = lax.axis_index("core").astype(jnp.int32)
    replica = (2 * lax.axis_index("x") + core).astype(jnp.int32)[None]
    core = core[None]
    slot_of = slot_table(owners, 3)

    pieces = split(grad_parts.reshape(512, 512))
    left, right_factor = call(
        left_kernel,
        [SMEM, *vmem(4)],
        [sds((3, 512, 512), bf16), sds((3, 64, 512), bf16)],
        (core, left_codes, left_scales.T, right_codes, right_scales.T),
    )
    parts = exchange(pieces.reshape(8, 256, 128), ("x", "core"))
    routed = call(
        route_kernel,
        [*vmem(2), ANY],
        sds((64, 1536), bf16),
        (parts, slot_of.reshape(1, 64), left),
    )
    arrived = exchange(routed.reshape(64, 2, 768), "fsdp").reshape(64, 1536)
    own = exchange(call(spread_kernel, vmem(1), sds((4, 768, 128), bf16), (arrived,)), "x")
    other = lax.ppermute(own, "core", [(0, 1), (1, 0)])
    half_grad = sds((3, 256, 512), bf16)
    small = sds((8, 128), f32)
    own_grad, own_pre, own_squares = call(
        own_kernel,
        vmem(3),
        [half_grad, sds((3, 256, 128), f32), small],
        (own, right_factor, left),
    )
    other_grad, pre, squares, grad_squares = call(
        other_kernel,
        vmem(5),
        [half_grad, sds((64, 1536), f32), small, small],
        (other, right_factor, left, own_pre, own_squares),
    )
    all_squares = exchange(squares.reshape(8, 1, 128), ("x", "core")).reshape(8, 128)
    right_new = call(
        right_kernel,
        [SMEM, *vmem(3)],
        sds((3, 64, 512), f32),
        (replica, own_grad, other_grad, right_stat),
    )
    scaled = call(
        scale_kernel, vmem(3), sds((64, 1536), bf16), (all_squares, grad_squares, pre)
    )
    returned = exchange(scaled.reshape(64, 2, 768), "fsdp").reshape(64, 1536)
    left_new = call(
        gram_left_kernel,
        [SMEM, SMEM, *vmem(3), ANY],
        sds((3, 64, 512), f32),
        (replica, core, own_grad, other_grad, left_stat, scaled),
    )
    new_weights = pl.pallas_call(
        final_kernel,
        out_shape=sds((64, 8, 64), f32),
        in_specs=vmem(3),
        out_specs=ANY,
        scratch_shapes=[pltpu.VMEM((64, 8, 64), f32), pltpu.SemaphoreType.DMA((CHUNKS,))],
        compiler_params=pltpu.CompilerParams(vmem_limit_bytes=VMEM_GRANT),
    )(returned, slot_of.reshape(64, 1), weights)
    return (new_weights, left_new, right_new)


def solution(mesh):
    grid = Mesh(mesh.devices.reshape(64, 4, 2), ("fsdp", "x", "core"))
    dp = ("x", "core")
    return jax.shard_map(
        local,
        mesh=grid,
        in_specs=(
            P(dp, None, "fsdp", None),
            P(None, "fsdp", dp),
            P("fsdp", dp, None),
            P("fsdp", dp, None),
            P("fsdp", None, None),
            P("fsdp", dp, None),
            P("fsdp", None),
            P("fsdp", dp),
            P(),
        ),
        out_specs=(P(None, "fsdp", dp), P("fsdp", dp, None), P("fsdp", dp, None)),
        check_vma=False,
    )
```

```python
import jax
import jax.numpy as jnp
from jax import lax
from jax.experimental import pallas as pl
from jax.experimental.pallas import tpu as pltpu
from jax.sharding import Mesh
from jax.sharding import PartitionSpec as P

stat_decay = 0.95
step_size = 0.5
epsilon = 1e-06

bf16 = jnp.bfloat16
f32 = jnp.float32
LANES = 128
VMEM_GRANT = 16 * 1024 * 1024


def iota(shape, dim):
    return lax.broadcasted_iota(jnp.int32, shape, dim)


def dot(a, b, ca=1, cb=0):
    return lax.dot_general(a, b, (((ca,), (cb,)), ((), ())), preferred_element_type=f32)


def onehot(mask):
    return jnp.where(mask, 1.0, 0.0).astype(bf16)


def natural_row(order, first_half):
    half = (order // 256 + first_half) % 2
    return 8 * (order % 64) + 4 * half + (order // 64) % 4


def vmem(n):
    return [pl.BlockSpec(memory_space=pltpu.VMEM)] * n


SMEM = pl.BlockSpec(memory_space=pltpu.SMEM)
ANY = pl.BlockSpec(memory_space=pl.ANY)


def call(kernel, ins, outs, args):
    single = not isinstance(outs, (list, tuple))
    shapes = [outs] if single else list(outs)
    got = pl.pallas_call(
        kernel,
        out_shape=shapes,
        in_specs=ins,
        out_specs=vmem(len(shapes)),
        compiler_params=pltpu.CompilerParams(vmem_limit_bytes=VMEM_GRANT),
    )(*args)
    return got[0] if single else got


def sds(shape, dtype):
    return jax.ShapeDtypeStruct(shape, dtype)


CHUNKS = 4


def split_kernel(x_ref, out_ref, buf, sem):
    rows = 512 // CHUNKS
    per = rows // 8

    def leaving(i):
        return pltpu.make_async_copy(buf.at[i], out_ref.at[:, :, pl.ds(per * i, per)], sem.at[i])

    order = iota((rows, rows), 0)
    half, r, block = order // (4 * per), (order // per) % 4, order % per
    perm = onehot(8 * block + 4 * half + r == iota((rows, rows), 1))
    for i in range(CHUNKS):
        moved = dot(perm, x_ref[rows * i : rows * i + rows]).astype(bf16)
        for x in range(4):
            for c in range(2):
                for r in range(4):
                    at = (4 * c + r) * per
                    piece = moved[at : at + per, LANES * x : LANES * x + LANES]
                    buf[i, 2 * x + c, r] = piece
        leaving(i).start()
    for i in range(CHUNKS):
        leaving(i).wait()


def split(x):
    return pl.pallas_call(
        split_kernel,
        out_shape=sds((8, 4, 64, 128), bf16),
        in_specs=vmem(1),
        out_specs=ANY,
        scratch_shapes=[
            pltpu.VMEM((CHUNKS, 8, 4, 64 // CHUNKS, 128), bf16),
            pltpu.SemaphoreType.DMA((CHUNKS,)),
        ],
        compiler_params=pltpu.CompilerParams(vmem_limit_bytes=VMEM_GRANT),
    )(x)


def route_kernel(parts_ref, slot_ref, after_ref, out_ref):
    total = parts_ref[0].astype(f32)
    for s in range(1, 8):
        total = total + parts_ref[s].astype(f32)
    total = total.astype(bf16)
    wide = jnp.concatenate([total[64 * r : 64 * r + 64] for r in range(4)], axis=1)
    slot = slot_ref[...]
    for k in range(3):
        pick = onehot(slot == 3 * iota((64, 64), 0) + k)
        out_ref[:, 512 * k : 512 * k + 512] = dot(pick, wide).astype(bf16)


def left_kernel(core_ref, lc_ref, ls_ref, rc_ref, rs_ref, out_ref, rf_ref):
    back = onehot(natural_row(iota((512, 512), 0), 0) == iota((512, 512), 1))
    cols = onehot(natural_row(iota((512, 512), 1), core_ref[0]) == iota((512, 512), 0))
    for k in range(3):
        factor = (lc_ref[k].astype(f32) * ls_ref[:, k : k + 1]).astype(bf16)
        rows = dot(back, factor).astype(bf16)
        out_ref[k] = dot(rows, cols).astype(bf16)
        rf_ref[k] = (rc_ref[k].astype(f32) * rs_ref[:, k : k + 1]).astype(bf16)


def tile_kernel(piece_ref, out_ref):
    for q in range(4):
        for kr in range(12):
            at = 192 * q + 16 * kr
            tile = piece_ref[16 * q : 16 * q + 16, LANES * kr : LANES * kr + LANES]
            out_ref[at : at + 16] = tile


def half_products(at, src_ref, rf_ref, left_ref, g_ref):
    lane = iota((8, LANES), 1)
    grad_squares = jnp.zeros((8, LANES), f32)
    products = []
    for k in range(3):
        for x in range(4):
            for q in range(4):
                for r in range(4):
                    row = 64 * r + 16 * q
                    g_ref[k, row : row + 16, LANES * x : LANES * x + LANES] = src_ref[
                        x, pl.ds(192 * q + 16 * (4 * k + r), 16)
                    ]
        g = g_ref[k]
        rf = rf_ref[k]
        wide = jnp.concatenate([rf, jnp.zeros((128, 512), bf16), rf], axis=0)
        mixed = dot(g, wide, 1, 1).astype(bf16)
        pre = dot(left_ref[k, :256, at : at + 256], mixed[:, :128])
        products.append(pre + dot(left_ref[k, 256:, at : at + 256], mixed[:, 128:]))
        gf = g.astype(f32)
        grad_squares = jnp.where(lane == k, jnp.sum(gf * gf), grad_squares)
    return products, grad_squares


def own_kernel(own_ref, rf_ref, left_ref, g_ref, p_ref, gs_ref):
    products, grad_squares = half_products(0, own_ref, rf_ref, left_ref, g_ref)
    for k in range(3):
        p_ref[k] = products[k]
    gs_ref[...] = grad_squares


def other_kernel(
    other_ref, rf_ref, left_ref, own_p_ref, own_gs_ref, g_ref, p_ref, sq_ref, gs_ref
):
    products, grad_squares = half_products(256, other_ref, rf_ref, left_ref, g_ref)
    lane = iota((8, LANES), 1)
    squares = jnp.zeros((8, LANES), f32)
    for k in range(3):
        pre = own_p_ref[k] + products[k]
        for t in range(4):
            at = 512 * k + LANES * t
            p_ref[:, at : at + LANES] = pre[64 * t : 64 * t + 64]
        squares = jnp.where(lane == k, jnp.sum(pre * pre), squares)
    sq_ref[...] = squares
    gs_ref[...] = own_gs_ref[...] + grad_squares


def scale_kernel(sq_ref, gs_ref, p_ref, out_ref):
    total = jnp.sum(sq_ref[...], axis=0, keepdims=True)
    ratio = step_size * jnp.sqrt(gs_ref[0:1, :]) * lax.rsqrt(total + epsilon)
    for k in range(3):
        span = slice(512 * k, 512 * k + 512)
        out_ref[:, span] = (p_ref[:, span] * ratio[:, k : k + 1]).astype(bf16)


def right_kernel(replica_ref, own_ref, other_ref, stat_ref, out_ref):
    pick = onehot(iota((64, 512), 1) == 64 * replica_ref[0] + iota((64, 512), 0))
    for k in range(3):
        g = jnp.concatenate([own_ref[k], other_ref[k]], axis=0)
        cols = dot(pick, g, 1, 1).astype(bf16)
        out_ref[k] = stat_decay * stat_ref[k] + (1.0 - stat_decay) * dot(cols, g)


def gram_left_kernel(
    replica_ref, core_ref, own_ref, other_ref, stat_ref, after_ref, out_ref
):
    core = core_ref[0]
    order = natural_row(iota((512, 512), 1), core)
    back = onehot(order == iota((512, 512), 0))
    mine = onehot(
        natural_row(iota((64, 512), 1), core) == 64 * replica_ref[0] + iota((64, 512), 0)
    )
    for k in range(3):
        g = jnp.concatenate([own_ref[k], other_ref[k]], axis=0)
        rows = dot(mine, g).astype(bf16)
        whole = dot(back, g).astype(bf16)
        out_ref[k] = stat_decay * stat_ref[k] + (1.0 - stat_decay) * dot(rows, whole, 1, 1)


def final_kernel(ret_ref, slot_ref, w_ref, out_ref, buf, sem):
    slot = slot_ref[...]
    update = jnp.zeros((64, 512), f32)
    for k in range(3):
        pick = onehot(slot == 3 * iota((64, 64), 1) + k)
        update = update + dot(pick, ret_ref[:, 512 * k : 512 * k + 512])
    per = 64 // CHUNKS

    def leaving(i):
        part = pl.ds(per * i, per)
        return pltpu.make_async_copy(buf.at[part], out_ref.at[part], sem.at[i])

    for i in range(CHUNKS):
        part = slice(per * i, per * i + per)
        for t in range(4):
            for half in range(2):
                row = 4 * half + t
                at = LANES * t + 64 * half
                buf[part, row, :] = w_ref[part, row, :] - update[part, at : at + 64]
        leaving(i).start()
    for i in range(CHUNKS):
        leaving(i).wait()


def slot_table(owners, capacity):
    count = owners.shape[0]
    index = jnp.arange(count, dtype=jnp.int32)
    earlier = (owners[:, None] == owners[None, :]) & (index[None, :] < index[:, None])
    rank = jnp.sum(earlier.astype(jnp.int32), axis=1)
    return owners * capacity + rank


def exchange(x, axis):
    return lax.all_to_all(x, axis, split_axis=0, concat_axis=0, tiled=True)


def local(
    grad_parts,
    weights,
    left_stat,
    right_stat,
    left_codes,
    right_codes,
    left_scales,
    right_scales,
    owners,
):
    core = lax.axis_index("core").astype(jnp.int32)
    replica = (2 * lax.axis_index("x") + core).astype(jnp.int32)[None]
    core = core[None]
    slot_of = slot_table(owners, 3)

    pieces = split(grad_parts.reshape(512, 512))
    left, right_factor = call(
        left_kernel,
        [SMEM, *vmem(4)],
        [sds((3, 512, 512), bf16), sds((3, 64, 512), bf16)],
        (core, left_codes, left_scales.T, right_codes, right_scales.T),
    )
    parts = exchange(pieces.reshape(8, 256, 128), ("x", "core"))
    routed = call(
        route_kernel,
        [*vmem(2), ANY],
        sds((64, 1536), bf16),
        (parts, slot_of.reshape(1, 64), left),
    )
    arrived = exchange(routed.reshape(64, 2, 768), "fsdp").reshape(64, 1536)
    piece = call(tile_kernel, vmem(1), sds((768, 128), bf16), (arrived,))
    own = lax.all_gather(piece, "x", axis=0, tiled=True).reshape(4, 768, 128)
    other = lax.ppermute(own, "core", [(0, 1), (1, 0)])
    half_grad = sds((3, 256, 512), bf16)
    small = sds((8, 128), f32)
    own_grad, own_pre, own_squares = call(
        own_kernel,
        vmem(3),
        [half_grad, sds((3, 256, 128), f32), small],
        (own, right_factor, left),
    )
    other_grad, pre, squares, grad_squares = call(
        other_kernel,
        vmem(5),
        [half_grad, sds((64, 1536), f32), small, small],
        (other, right_factor, left, own_pre, own_squares),
    )
    all_squares = exchange(squares.reshape(8, 1, 128), ("x", "core")).reshape(8, 128)
    right_new = call(
        right_kernel,
        [SMEM, *vmem(3)],
        sds((3, 64, 512), f32),
        (replica, own_grad, other_grad, right_stat),
    )
    scaled = call(
        scale_kernel, vmem(3), sds((64, 1536), bf16), (all_squares, grad_squares, pre)
    )
    returned = exchange(scaled.reshape(64, 2, 768), "fsdp").reshape(64, 1536)
    left_new = call(
        gram_left_kernel,
        [SMEM, SMEM, *vmem(3), ANY],
        sds((3, 64, 512), f32),
        (replica, core, own_grad, other_grad, left_stat, scaled),
    )
    new_weights = pl.pallas_call(
        final_kernel,
        out_shape=sds((64, 8, 64), f32),
        in_specs=vmem(3),
        out_specs=ANY,
        scratch_shapes=[pltpu.VMEM((64, 8, 64), f32), pltpu.SemaphoreType.DMA((CHUNKS,))],
        compiler_params=pltpu.CompilerParams(vmem_limit_bytes=VMEM_GRANT),
    )(returned, slot_of.reshape(64, 1), weights)
    return (new_weights, left_new, right_new)


def solution(mesh):
    grid = Mesh(mesh.devices.reshape(64, 4, 2), ("fsdp", "x", "core"))
    dp = ("x", "core")
    return jax.shard_map(
        local,
        mesh=grid,
        in_specs=(
            P(dp, None, "fsdp", None),
            P(None, "fsdp", dp),
            P("fsdp", dp, None),
            P("fsdp", dp, None),
            P("fsdp", None, None),
            P("fsdp", dp, None),
            P("fsdp", None),
            P("fsdp", dp),
            P(),
        ),
        out_specs=(P(None, "fsdp", dp), P("fsdp", dp, None), P("fsdp", dp, None)),
        check_vma=False,
    )
```
